128 devices in a mesh: dp: 16 (over z, x_hi, core), mp: 8 (over x_lo, y).
Axes of the slice: x: 4 (x_hi: 2, x_lo: 2; x = x_hi * 2 + x_lo), y: 4, z: 4, core: 2. Of those that a mesh axis runs over, the one named last changes fastest.
Arguments:
- patches: bfloat16 [512, 256, 1280], P(('dp', 'mp')), may hold values from -6 to 6
- position: bfloat16 [256, 1280], replicated, may hold values from -3 to 3
- keep: int32 [512, 64], P(('dp', 'mp')), may hold values from 0 to 255, as said below
- counts: int32 [512], replicated, may hold values from 1 to 64, as said below
- offsets: int32 [512], replicated, may hold values from 0 to 20479, as said below
- ln_gain: float32 [1, 2, 1280], replicated, may hold values from 0.25 to 1.75
- ln_bias: float32 [1, 2, 1280], replicated, may hold values from -2 to 2
- w_qkv: bfloat16 [1, 3, 1280, 1280], P(None, None, 'dp', 'mp')
- b_qkv: float32 [1, 3, 1280], P(None, None, 'mp'), may hold values from -3 to 3
- w_o: bfloat16 [1, 1280, 1280], P(None, 'mp', 'dp'), may hold values from -0.15625 to 0.15625
- b_o: float32 [1, 1280], replicated, may hold values from -1.5 to 1.5
- w_up: bfloat16 [1, 1280, 5120], P(None, 'dp', 'mp'), may hold values from -0.15625 to 0.15625
- b_up: float32 [1, 5120], P(None, 'mp'), may hold values from -3 to 3
- w_down: bfloat16 [1, 5120, 1280], P(None, 'mp', 'dp'), may hold values from -0.078125 to 0.078125
- b_down: float32 [1, 1280], replicated, may hold values from -1.5 to 1.5
Outputs:
- encoded: bfloat16 [20480, 1280], P(('dp', 'mp'))
The draws below stay inside these ranges and needn't reach their ends.
Inputs may be any that keep to these rules, and one draw needn't show every extreme that they name: `keep`: the first counts[i] entries of row i are distinct and name image i's visible patches; later entries are unused. `counts`: some image has exactly 64 visible patches. Image i, held by dp index s = i // 32, occupies packed rows offsets[i] to offsets[i] + counts[i] - 1, all inside the aligned block of 80 rows numbered d * 16 + s for some shard d; no two images share a row.
All inputs are finite; a program needn't handle non-finite values.
Results may differ from the reference program's by a relative error of at most 0.015.
Values may be sent and summed in bfloat16 or wider, within the bound.
A program may use at most 64 MiB of HBM per device.

```python
import math
import jax
import jax.numpy as jnp
from jax import lax

D = 1280
HEADS = 16
HEAD = 80
FF = 5120
PATCHES = 256
KEEP_MAX = 64
LAYERS = 1
IMG_DEV = 32
IMAGES = 512
SLOT = 80
PACK_DEV = 1280
PACKED = 20480
N_MP = 8


def packing_plan(key):
    shard_total = IMAGES // IMG_DEV
    key_order, key_raw, key_cap, key_force = jax.random.split(jax.random.fold_in(key, 71), 4)
    order = jax.vmap(lambda subkey: jax.random.permutation(subkey, IMG_DEV))(jax.random.split(key_order, shard_total)).astype(jnp.int32)
    destination = order % shard_total
    rank_in = order // shard_total
    lowest = max(1, KEEP_MAX // 8)
    ceiling = jax.random.randint(key_cap, (shard_total, 1), lowest, KEEP_MAX + 1)
    raw_count = jnp.minimum(jax.random.randint(key_raw, (shard_total, IMG_DEV), lowest, KEEP_MAX + 1), ceiling)
    mates = destination[:, :, None] == destination[:, None, :]
    mate_total = jnp.sum(jnp.where(mates, raw_count[:, None, :], 0), axis=-1)
    mate_number = jnp.sum(mates.astype(jnp.int32), axis=-1)
    room = SLOT - mate_number
    scaled = 1 + (raw_count - 1) * room // jnp.maximum(mate_total - mate_number, room)
    forced_source = jax.random.randint(key_force, (), 0, shard_total)
    source_ids = jnp.arange(shard_total, dtype=jnp.int32)[:, None]
    in_source = source_ids == forced_source
    chosen = in_source & (order == 0)
    partner = in_source & (destination == 0)
    counts_grid = jnp.where(chosen, KEEP_MAX, jnp.where(partner, 1, scaled))
    earlier = mates & (rank_in[:, None, :] < rank_in[:, :, None])
    before = jnp.sum(jnp.where(earlier, counts_grid[:, None, :], 0), axis=-1)
    offsets_grid = destination * PACK_DEV + source_ids * SLOT + before
    return (counts_grid.reshape(IMAGES).astype(jnp.int32), offsets_grid.reshape(IMAGES).astype(jnp.int32))


def draw_counts(key, part):
    return packing_plan(key)[0]


def draw_offsets(key, part):
    return packing_plan(key)[1]


def draw_keep(key, part):
    subkeys = jax.random.split(jax.random.fold_in(key, 13), IMAGES)
    return jax.vmap(lambda subkey: jax.random.permutation(subkey, PATCHES)[:KEEP_MAX])(subkeys).astype(jnp.int32)


def draw_w_qkv(key, part):
    key_base = jax.random.fold_in(jax.random.fold_in(key, 29), 0)
    matrices = jax.random.normal(key_base, (LAYERS, 3, D, D), jnp.float32) / math.sqrt(D)
    return matrices.astype(jnp.bfloat16)


def levels(rng, extent, cuts, low, largest):
    level, own = 1.0, jax.random.fold_in(rng, 6)
    for dim, blocks in cuts:
        steps = jnp.exp(jax.random.uniform(jax.random.fold_in(own, dim), (blocks,), jnp.float32, low / len(cuts), largest / len(cuts)))
        level = level * jnp.repeat(steps, extent[dim] // blocks).reshape([-1 if axis == dim else 1 for axis in range(len(extent))])
    return level


def bell_draw(rng, extent, deviation, limit, cuts=(), kind=jnp.bfloat16):
    result = jax.random.normal(rng, extent, jnp.float32) * deviation
    if len(cuts) > 0:
        result = levels(rng, extent, cuts, -0.22, 0.18) * result
    return jnp.clip(result, min=-limit, max=limit).astype(kind)


def setup_inputs(seed: int = 0) -> dict:
    keys = jax.random.split(jax.random.key(seed), 16)
    return {
        "patches": bell_draw(keys[0], (IMAGES, PATCHES, D), 1.0, 6.0, ((0, 128),)),
        "position": bell_draw(keys[1], (PATCHES, D), 0.5, 3.0),
        "keep": draw_keep(jax.random.fold_in(keys[15], 71), 0),
        "counts": draw_counts(jax.random.fold_in(keys[15], 71), 0),
        "offsets": draw_offsets(jax.random.fold_in(keys[15], 71), 0),
        "ln_gain": jnp.clip(1.0 + 0.15 * jax.random.normal(keys[5], (LAYERS, 2, D), jnp.float32), 0.25, 1.75),
        "ln_bias": bell_draw(keys[6], (LAYERS, 2, D), 0.3, 2.0, (), jnp.float32),
        "w_qkv": draw_w_qkv(jax.random.fold_in(keys[15], 71), 0),
        "b_qkv": bell_draw(keys[8], (LAYERS, 3, D), 0.5, 3.0, ((2, 8),), jnp.float32),
        "w_o": bell_draw(keys[9], (LAYERS, D, D), D ** -0.5, 0.15625, ((1, 8), (2, 16))),
        "b_o": bell_draw(keys[10], (LAYERS, D), 0.2, 1.5, (), jnp.float32),
        "w_up": bell_draw(keys[11], (LAYERS, D, FF), D ** -0.5, 0.15625, ((1, 16), (2, 8))),
        "b_up": bell_draw(keys[12], (LAYERS, FF), 0.5, 3.0, ((1, 8),), jnp.float32),
        "w_down": bell_draw(keys[13], (LAYERS, FF, D), FF ** -0.5, 0.078125, ((1, 8), (2, 16))),
        "b_down": bell_draw(keys[14], (LAYERS, D), 0.2, 1.5, (), jnp.float32),
    }


def layer_norm(values, gain_row, shift_row):
    row_mean = lax.optimization_barrier(jnp.mean(values, axis=-1, keepdims=True))
    centred = values - row_mean
    spread = lax.optimization_barrier(jnp.mean(centred * centred, axis=-1, keepdims=True))
    return (centred * lax.rsqrt(spread + 1e-06) * gain_row + shift_row).astype(jnp.bfloat16)

def split_sum(left, weight, groups):
    group_width = left.shape[1] // groups
    running = jnp.zeros((left.shape[0], weight.shape[1]), jnp.float32)
    for group_index in range(groups):
        partial_value = jnp.dot(left[:, group_index * group_width:(group_index + 1) * group_width], weight[group_index * group_width:(group_index + 1) * group_width], preferred_element_type=jnp.float32)
        rounded = lax.optimization_barrier(partial_value.astype(jnp.bfloat16))
        running = running + rounded.astype(jnp.float32)
    return running

def shard_attention(pieces):
    queries, key_rows, value_rows, labels_shard = pieces
    scores = jnp.einsum('qhe,khe->hqk', queries.astype(jnp.float32), key_rows.astype(jnp.float32)) * (1.0 / math.sqrt(HEAD))
    matches = labels_shard[:, None] == labels_shard[None, :]
    scores = jnp.where(matches[None], scores, -jnp.inf)
    row_max = lax.optimization_barrier(jnp.max(scores, axis=-1, keepdims=True))
    weights = jnp.exp(scores - row_max)
    probabilities = (weights / lax.optimization_barrier(jnp.sum(weights, axis=-1, keepdims=True))).astype(jnp.bfloat16)
    attended = jnp.einsum('hqk,khe->qhe', probabilities.astype(jnp.float32), value_rows.astype(jnp.float32))
    return attended.astype(jnp.bfloat16)

def reference(patches, position, keep, counts, offsets, ln_gain, ln_bias, w_qkv, b_qkv, w_o, b_o, w_up, b_up, w_down, b_down):
    picked = jnp.take_along_axis(patches, keep[:, :, None], axis=1)
    placed = jnp.take(position, keep, axis=0)
    tokens = (picked.astype(jnp.float32) + placed.astype(jnp.float32)).astype(jnp.bfloat16)
    positions_in = jnp.arange(KEEP_MAX, dtype=jnp.int32)
    is_live = positions_in[None, :] < counts[:, None]
    target = jnp.where(is_live, offsets[:, None] + positions_in[None, :], PACKED).reshape(-1)
    stream = jnp.zeros((PACKED, D), jnp.bfloat16).at[target].set(tokens.reshape(-1, D), mode='drop')
    packed_rows = jnp.arange(PACKED, dtype=jnp.int32)
    image_ids = jnp.arange(counts.shape[0], dtype=jnp.int32)
    inside = (packed_rows[:, None] >= offsets[None, :]) & (packed_rows[:, None] < (offsets + counts)[None, :])
    labels = lax.optimization_barrier(jnp.max(jnp.where(inside, image_ids[None, :] + 1, 0), axis=1)) - 1
    shard_total = PACKED // PACK_DEV
    for layer_index in range(LAYERS):
        normed = layer_norm(stream.astype(jnp.float32), ln_gain[layer_index, 0], ln_bias[layer_index, 0])
        projected = (jnp.einsum('rd,tdc->trc', normed.astype(jnp.float32), w_qkv[layer_index].astype(jnp.float32)) + b_qkv[layer_index][:, None, :]).astype(jnp.bfloat16)
        shaped = projected.reshape(3, shard_total, PACK_DEV, HEADS, HEAD)
        attended = lax.map(shard_attention, (shaped[0], shaped[1], shaped[2], labels.reshape(shard_total, PACK_DEV)))
        attended = attended.reshape(PACKED, D)
        residual = stream.astype(jnp.float32) + split_sum(attended, w_o[layer_index], N_MP) + b_o[layer_index]
        normed_mlp = layer_norm(residual, ln_gain[layer_index, 1], ln_bias[layer_index, 1])
        up_proj = jnp.dot(normed_mlp, w_up[layer_index], preferred_element_type=jnp.float32) + b_up[layer_index]
        hidden = jax.nn.gelu(up_proj, approximate=False).astype(jnp.bfloat16)
        stream = (residual + split_sum(hidden, w_down[layer_index], N_MP) + b_down[layer_index]).astype(jnp.bfloat16)
    return jnp.where(labels[:, None] >= 0, stream, jnp.zeros_like(stream))
```

```python
import jax
import jax.numpy as jnp
from jax import lax
from jax.experimental import pallas as pl
from jax.experimental.pallas import tpu as pltpu
from jax.sharding import PartitionSpec as P

BF = jnp.bfloat16
F32 = jnp.float32
MESH = pl.DeviceIdType.MESH
ALL = slice(None)
D = 1280
HEAD = 80
SLOT = 80
ROWS = 160
KEEP = 64
SCALE = 1.0 / HEAD**0.5

ORDERS = ("xyz", "yzx", "zxy")
SECTIONS = (
    ((0, 256), (640, 256), (1280, 128)),
    ((256, 256), (896, 128), (1408, 256)),
    ((512, 128), (1024, 256), (1664, 256)),
)
LANES = 1920
N_SEM = 124


def place():
    dp, mp = lax.axis_index("dp"), lax.axis_index("mp")
    return {
        "x": lax.rem(dp // 2, 2) * 2 + mp // 4,
        "y": lax.rem(mp, 4),
        "z": dp // 4,
        "c": lax.rem(dp, 2),
    }


def device(p):
    return (p["z"] * 4 + (p["x"] // 2) * 2 + p["c"], lax.rem(p["x"], 2) * 4 + p["y"])


def shifted(p, dim, by):
    return {**p, dim: lax.rem(p[dim] + by + 4, 4)}


def other_core(p):
    return {**p, "c": 1 - p["c"]}


def slab(colour, phase, p, half=None):
    free = ORDERS[colour][: phase - 1]
    at = {"xl": lax.rem(p["x"], 2), "xh": p["x"] // 2, "y": p["y"], "z": p["z"], "r": ALL}
    for dim in free:
        for part in ("xl", "xh") if dim == "x" else (dim,):
            at[part] = ALL
    if half is not None:
        if phase == 1:
            at["r"] = pl.ds(0, 48) if half == 0 else pl.ds(48, 32)
        else:
            part, count = ("xl", 1) if free[0] == "x" else (free[0], 2)
            at[part] = pl.ds(half * count, count)
    return (at["xl"], at["y"], at["z"], at["xh"], p["c"], at["r"])


class Transfer:
    def __init__(self, owner, sent, received, lanes, target):
        number = owner.count
        owner.count += 1
        self.owner = owner

        def copy(where):
            ref = owner.ref.at[where + (pl.ds(*lanes),)]
            return pltpu.make_async_remote_copy(
                src_ref=ref,
                dst_ref=ref,
                send_sem=owner.send.at[number],
                recv_sem=owner.recv.at[number],
                device_id=device(target),
                device_id_type=MESH,
            )

        self.out, self.into = copy(sent), copy(received)

    def start(self):
        self.out.start()
        self.owner.started.append(self.out)

    def wait(self):
        self.into.wait_recv()


class Gather:
    def __init__(self, p, ref, send, recv):
        self.p, self.ref, self.send, self.recv = p, ref, send, recv
        self.count, self.started = 0, []
        mate = other_core(p)
        self.own = Transfer(self, slab(0, 1, p), slab(0, 1, mate), (0, LANES), mate)
        self.first = [self.phase(k, 1, (640 * k, 640)) for k in range(3)]
        self.second = [self.phase(k, 2, (640 * k, 640)) for k in range(3)]
        self.third = [[self.phase(k, 3, s[k]) for k in range(3)] for s in SECTIONS]

    def phase(self, k, number, lanes):
        p = self.p
        dim = ORDERS[k][number - 1]
        up, down, far = shifted(p, dim, 1), shifted(p, dim, -1), shifted(p, dim, 2)
        mate = other_core(p)

        def at(q, half=None):
            return slab(k, number, q, half)

        def copy(sent, received, target):
            return Transfer(self, sent, received, lanes, target)

        return {
            "full_up": copy(at(p), at(down), up),
            "full_down": copy(at(p), at(up), down),
            "half_up": copy(at(down, 0), at(far, 0), up),
            "half_down": copy(at(up, 1), at(far, 1), down),
            "mate_down": copy(at(down), at(other_core(down)), mate),
            "mate_up": copy(at(up), at(other_core(up)), mate),
            "mate_far0": copy(at(far, 0), at(other_core(far), 0), mate),
            "mate_far1": copy(at(far, 1), at(other_core(far), 1), mate),
        }

    def fulls(self, group):
        for f in group:
            f["full_up"].start()
            f["full_down"].start()

    def halves(self, group):
        for f in group:
            f["full_up"].wait()
            f["half_up"].start()
            f["full_down"].wait()
            f["half_down"].start()
        for f in group:
            f["mate_down"].start()
            f["mate_up"].start()

    def far(self, group):
        for f in group:
            f["half_up"].wait()
            f["half_down"].wait()

    def far_to_mate(self, group):
        for f in group:
            f["mate_far0"].start()
            f["mate_far1"].start()

    def from_mate(self, group):
        for f in group:
            for name in ("mate_down", "mate_up", "mate_far0", "mate_far1"):
                f[name].wait()


def norm(values, gain, shift):
    mean = jnp.mean(values, axis=-1, keepdims=True)
    centred = values - mean
    spread = jnp.mean(centred * centred, axis=-1, keepdims=True)
    return (centred * lax.rsqrt(spread + 1e-06) * gain + shift).astype(BF)


def dot(a, b, contract=((1,), (0,))):
    return lax.dot_general(a, b, (contract, ((), ())), preferred_element_type=F32)


NT = ((1,), (1,))
TN = ((0,), (0,))


def kernel(
    patches,
    position,
    keep,
    counts,
    offsets,
    ln_gain,
    ln_bias,
    w_qkv,
    b_qkv,
    w_o,
    b_o,
    w_up,
    b_up,
    w_down,
    b_down,
    out,
    w,
    pictures,
    places,
    tokens,
    arrived,
    chosen,
    spread,
    stream,
    normed,
    residual,
    hidden,
    biases,
    send,
    recv,
    load,
    send1,
    recv1,
    send1e,
    recv1e,
    sendb,
    recvb,
    send2,
    recv2,
    send2e,
):
    dp, mp = lax.axis_index("dp"), lax.axis_index("mp")
    p = place()
    mate = other_core(p)
    half = lax.rem(dp, 2)
    tail_owner = (lax.rem(dp, 8), lax.rem(dp + 4, 8))
    has_tail = (mp == tail_owner[0]) | (mp == tail_owner[1])
    tail_tile = jnp.where(mp == tail_owner[0], 8, 9)
    goes_home = mp == dp // 2

    arrived[:, :, 128:256] = jnp.zeros((8, 256, 128), BF)

    barrier = pltpu.get_barrier_semaphore()

    def greet(target):
        pl.semaphore_signal(barrier, inc=1, device_id=target, device_id_type=MESH)

    for q in [shifted(p, d, s) for d in "xyz" for s in (1, -1)] + [mate]:
        greet(device(q))
    for k in range(1, 8):
        greet((dp, lax.rem(mp + k, 8)))
    for k in range(2):
        for m in range(8):
            source = mp * 2 + k

            @pl.when(jnp.logical_not((source == dp) & (mp == m)))
            def _():
                greet((source, jnp.int32(m)))

    load_pictures = pltpu.make_async_copy(patches, pictures, load.at[0])
    load_places = pltpu.make_async_copy(position, places, load.at[1])
    load_pictures.start()
    load_places.start()

    xl, xh = lax.rem(p["x"], 2), p["x"] // 2
    mine = (xl, p["y"], p["z"], xh, p["c"], ALL)

    def put(lane, value):
        w[mine + (pl.ds(lane, value.shape[1]),)] = value.astype(BF)

    eye = (
        lax.broadcasted_iota(jnp.int32, (SLOT, SLOT), 0)
        == lax.broadcasted_iota(jnp.int32, (SLOT, SLOT), 1)
    ).astype(F32).astype(BF)
    out_t = dot(eye, w_o[0], NT)
    down_t = dot(eye, w_down[0], NT)
    qkv = [w_qkv[0, t].astype(F32) for t in range(3)]
    put(0, qkv[0][:, :128])
    put(128, qkv[1][:, :128])
    put(640, qkv[2][:, :128])
    put(768, jnp.concatenate([v[:, 128:160] for v in qkv] + [out_t[:, 128:160]], axis=1))
    put(1280, out_t[:, :128])
    put(256, w_up[0, :, 0:256])
    put(896, w_up[0, :, 256:384])
    put(1408, w_up[0, :, 384:640])
    put(512, down_t[:, 0:128])
    put(1024, down_t[:, 128:384])
    put(1664, down_t[:, 384:640])

    for t in range(3):
        biases[mp, t : t + 1, :] = b_qkv[0, t : t + 1, 0:128]
    biases[mp, 3:4, :] = jnp.concatenate(
        [b_qkv[0, t : t + 1, 128:160] for t in range(3)] + [jnp.zeros((1, 32), F32)], axis=1
    )
    for t in range(5):
        biases[mp, 4 + t : 5 + t, :] = b_up[0:1, t * 128 : (t + 1) * 128]

    load_pictures.wait()
    load_places.wait()
    for i in range(4):
        hit = lax.broadcasted_iota(jnp.int32, (256, KEEP), 0) == keep[i : i + 1, :]
        hit = hit.astype(F32).astype(BF)
        picked = dot(hit, pictures[i], TN) + dot(hit, places[...], TN)
        tokens[i * KEEP : (i + 1) * KEEP, :] = picked.astype(BF)

    pl.semaphore_wait(barrier, 30 - goes_home.astype(jnp.int32))

    g = Gather(p, w, send, recv)
    g.fulls(g.first)
    g.own.start()

    def tile(k):
        return pl.ds(pl.multiple_of(k * 128, 128), 128)

    first_sends = []
    for k in range(1, 8):
        peer = lax.rem(mp + k, 8)
        for src, dst, s, r in (
            (tokens.at[:, tile(peer)], arrived.at[mp, :, pl.ds(0, 128)], send1, recv1),
            (biases.at[mp], biases.at[mp], sendb, recvb),
        ):
            copy = pltpu.make_async_remote_copy(
                src_ref=src,
                dst_ref=dst,
                send_sem=s.at[k],
                recv_sem=r.at[mp],
                device_id=(dp, peer),
                device_id_type=MESH,
            )
            copy.start()
            first_sends.append(copy)
    tail_sends = []
    for k in range(2):
        copy = pltpu.make_async_remote_copy(
            src_ref=tokens.at[:, pl.ds(1024 + 128 * k, 128)],
            dst_ref=arrived.at[mp, :, pl.ds(128, 128)],
            send_sem=send1e.at[k],
            recv_sem=recv1e.at[mp],
            device_id=(dp, tail_owner[k]),
            device_id_type=MESH,
        )
        tail_sends.append(copy)

        @pl.when(mp != tail_owner[k])
        def _():
            copy.start()

        @pl.when(mp == tail_owner[k])
        def _():
            arrived[mp, :, 128:256] = tokens[:, 1024 + 128 * k : 1152 + 128 * k]

    arrived[mp, :, 0:128] = tokens[:, tile(mp)]

    lane = lax.broadcasted_iota(jnp.int32, (16, 128), 1)
    inner = jnp.where(lane < KEEP, lane, lane - KEEP)
    pieces = []
    for k in range(16):
        a, b = dp * 32 + 2 * k, dp * 32 + 2 * k + 1
        count = jnp.where(lane < KEEP, counts[a], counts[b])
        start = jnp.where(lane < KEEP, offsets[a], offsets[b])
        pieces.append(jnp.where(inner < count, start + inner, -1))
    goal = jnp.concatenate(pieces, axis=1)
    sub = lax.broadcasted_iota(jnp.int32, (16, 2048), 0)

    def choose(i, carry):
        shard = i // 5
        row = shard * 1280 + dp * SLOT + (i - shard * 5) * 16
        hit = (goal - row) == sub
        chosen[pl.ds(pl.multiple_of(i * 16, 16), 16), :] = hit.astype(F32).astype(BF)
        return carry

    lax.fori_loop(0, 40, choose, 0)
    g.halves(g.first)
    lax.fori_loop(40, 80, choose, 0)

    labels_row, labels_col = [], []
    for h in range(2):
        first = dp * 1280 + (mp * 2 + h) * SLOT
        down = first + lax.broadcasted_iota(jnp.int32, (SLOT, 128), 0)
        across = first + lax.broadcasted_iota(jnp.int32, (SLOT, 128), 1)

        def mark(i, carry):
            image = (mp * 2 + h) * 32 + i
            low = offsets[image]
            high = low + counts[image]
            return tuple(
                jnp.where((rows >= low) & (rows < high), i + 1, old)
                for rows, old in zip((down, across), carry)
            )

        zero = jnp.zeros((SLOT, 128), jnp.int32)
        col, row = lax.fori_loop(0, 32, mark, (zero, zero))
        labels_col.append(col)
        labels_row.append(row)
    same = [(labels_col[h] == labels_row[h])[:, :SLOT] for h in range(2)]
    used = jnp.concatenate([labels_col[h][:, 0:1] for h in range(2)], axis=0) > 0

    g.far(g.first)
    g.fulls(g.second)
    g.far_to_mate(g.first)

    def wait_first(ref, sem, source):
        pltpu.make_async_remote_copy(
            src_ref=ref,
            dst_ref=ref,
            send_sem=send1.at[0],
            recv_sem=sem.at[source],
            device_id=(dp, source),
            device_id_type=MESH,
        ).wait_recv()

    for k in range(1, 8):
        source = lax.rem(mp + k, 8)
        wait_first(arrived.at[source, :, pl.ds(0, 128)], recv1, source)

    @pl.when(has_tail)
    def _():
        for k in range(1, 8):
            source = lax.rem(mp + k, 8)
            wait_first(arrived.at[source, :, pl.ds(128, 128)], recv1e, source)

    group = arrived[...].reshape(2048, 256)
    for k in range(4):
        rows = pl.ds(k * 320, 320)
        spread[rows, :] = dot(chosen[rows, :], group).astype(BF)

    g.halves(g.second)

    def slot_rows(k):
        return pl.ds(pl.multiple_of(k * SLOT, 16), SLOT)

    second_sends = []
    for k in range(16):
        shard = lax.rem(dp + k, 16)
        for extra in range(2):
            where = tail_tile if extra else mp
            copy = pltpu.make_async_remote_copy(
                src_ref=spread.at[slot_rows(shard), pl.ds(128 * extra, 128)],
                dst_ref=stream.at[slot_rows(half), tile(where)],
                send_sem=(send2e if extra else send2).at[k],
                recv_sem=recv2.at[half, where],
                device_id=(shard, dp // 2),
                device_id_type=MESH,
            )
            away = jnp.logical_not(goes_home) if k == 0 else None
            if extra:
                away = has_tail if away is None else has_tail & away
            if away is None:
                copy.start()
            else:
                pl.when(away)(copy.start)
            second_sends.append((copy, away))

    @pl.when(goes_home)
    def _():
        stream[slot_rows(half), tile(mp)] = spread[slot_rows(dp), 0:128]

    @pl.when(goes_home & has_tail)
    def _():
        stream[slot_rows(half), tile(tail_tile)] = spread[slot_rows(dp), 128:256]

    g.far(g.second)
    g.fulls(g.third[0])
    g.fulls(g.third[1])
    g.far_to_mate(g.second)

    for h in range(2):
        source = mp * 2 + h
        for t in range(10):
            owner = t if t < 8 else lax.rem(source + (t - 8) * 4, 8)

            @pl.when(jnp.logical_not((source == dp) & (mp == owner)))
            def _():
                ref = stream.at[pl.ds(h * SLOT, SLOT), pl.ds(t * 128, 128)]
                pltpu.make_async_remote_copy(
                    src_ref=ref,
                    dst_ref=ref,
                    send_sem=send1.at[0],
                    recv_sem=recv2.at[h, t],
                    device_id=(dp, mp),
                    device_id_type=MESH,
                ).wait_recv()

    for k in range(1, 8):
        source = lax.rem(mp + k, 8)
        wait_first(biases.at[source], recvb, source)

    rows_in = stream[...].astype(F32)
    normed[...] = norm(rows_in, ln_gain[0, 0:1, :], ln_bias[0, 0:1, :])
    residual[...] = rows_in + b_o[...]

    g.halves(g.third[0])
    g.fulls(g.third[2])
    g.halves(g.third[1])
    g.far(g.third[0])
    g.far_to_mate(g.third[0])
    g.own.wait()
    g.from_mate(g.first)
    g.from_mate(g.second)
    g.from_mate(g.third[0])

    def weights(m, *lanes):
        parts = [w[m // 4, lax.rem(m, 4), :, :, :, :, pl.ds(*v)].reshape(D, v[1]) for v in lanes]
        return parts[0] if len(parts) == 1 else jnp.concatenate(parts, axis=1)

    def attention(m, carry):
        rows = normed[...]
        bias = biases[m]

        def projected(lanes, t):
            both = dot(rows, weights(m, lanes))
            return [both[:, 128 * i : 128 * (i + 1)] + bias[t + i : t + i + 1, :] for i in range(2)]

        q, k = projected((0, 256), 0)
        v, tail = projected((640, 256), 2)
        heads = []
        for i, value in enumerate((q, k, v)):
            second = jnp.concatenate([value[:, 80:128], tail[:, 32 * i : 32 * i + 32]], axis=1)
            heads.append((value[:, :80].astype(BF), second.astype(BF)))
        mixed = []
        for n in range(2):
            blocks = []
            for h in range(2):
                part = slice(h * SLOT, (h + 1) * SLOT)
                scores = dot(heads[0][n][part], heads[1][n][part], NT) * SCALE
                scores = jnp.where(same[h], scores, -jnp.inf)
                raised = jnp.exp(scores - jnp.max(scores, axis=-1, keepdims=True))
                share = (raised / jnp.sum(raised, axis=-1, keepdims=True)).astype(BF)
                blocks.append(dot(share, heads[2][n][part]))
            mixed.append(jnp.concatenate(blocks, axis=0))
        left = jnp.concatenate([mixed[0], mixed[1][:, :48]], axis=1).astype(BF)
        right = jnp.concatenate([jnp.zeros((ROWS, 96), F32), mixed[1][:, 48:]], axis=1).astype(BF)
        both = jnp.concatenate([left, right], axis=1)
        residual[...] += dot(both, weights(m, (1280, 128), (768, 128)), NT)
        return carry

    lax.fori_loop(0, 8, attention, 0)
    normed[...] = norm(residual[...], ln_gain[0, 1:2, :], ln_bias[0, 1:2, :])
    residual[...] += b_down[...]

    g.halves(g.third[2])
    g.far(g.third[1])
    g.far_to_mate(g.third[1])
    g.from_mate(g.third[1])

    def up(m, carry):
        rows = normed[...]
        bias = biases[m]
        for lanes, first in (((256, 256), 0), ((896, 128), 2), ((1408, 256), 3)):
            value = dot(rows, weights(m, lanes))
            row = jnp.concatenate(
                [bias[4 + first + i : 5 + first + i, :] for i in range(lanes[1] // 128)], axis=1
            )
            value = value + row
            value = 0.5 * value * (1.0 + lax.erf(value * (0.5**0.5)))
            hidden[m, :, first * 128 : first * 128 + lanes[1]] = value.astype(BF)
        return carry

    lax.fori_loop(0, 8, up, 0)

    g.far(g.third[2])
    g.far_to_mate(g.third[2])
    g.from_mate(g.third[2])

    def down(m, carry):
        residual[...] += dot(
            hidden[m], weights(m, (512, 128), (1024, 256), (1664, 256)), NT
        )
        return carry

    lax.fori_loop(0, 8, down, 0)
    out[...] = jnp.where(used, residual[...], 0.0).astype(BF)

    for copy in g.started + first_sends:
        copy.wait_send()
    for k in range(2):
        pl.when(mp != tail_owner[k])(tail_sends[k].wait_send)
    for copy, away in second_sends:
        if away is None:
            copy.wait_send()
        else:
            pl.when(away)(copy.wait_send)


def per_device(*args):
    vmem = pl.BlockSpec(memory_space=pltpu.VMEM)
    smem = pl.BlockSpec(memory_space=pltpu.SMEM)
    anywhere = pl.BlockSpec(memory_space=pl.ANY)
    specs = [anywhere, anywhere, vmem, smem, smem] + [vmem] * 10
    dma = pltpu.SemaphoreType.DMA
    return pl.pallas_call(
        kernel,
        out_shape=jax.ShapeDtypeStruct((ROWS, D), BF),
        in_specs=specs,
        out_specs=vmem,
        scratch_shapes=[
            pltpu.VMEM((2, 4, 4, 2, 2, SLOT, LANES), BF),
            pltpu.VMEM((4, 256, D), BF),
            pltpu.VMEM((256, D), BF),
            pltpu.VMEM((256, D), BF),
            pltpu.VMEM((8, 256, 256), BF),
            pltpu.VMEM((1280, 2048), BF),
            pltpu.VMEM((1280, 256), BF),
            pltpu.VMEM((ROWS, D), BF),
            pltpu.VMEM((ROWS, D), BF),
            pltpu.VMEM((ROWS, D), F32),
            pltpu.VMEM((8, ROWS, 640), BF),
            pltpu.VMEM((8, 16, 128), F32),
            dma((N_SEM,)),
            dma((N_SEM,)),
            dma((2,)),
            dma((8,)),
            dma((8,)),
            dma((2,)),
            dma((8,)),
            dma((8,)),
            dma((8,)),
            dma((16,)),
            dma((2, 10)),
            dma((16,)),
        ],
        compiler_params=pltpu.CompilerParams(
            collective_id=0, has_side_effects=True, vmem_limit_bytes=62 * 1024 * 1024
        ),
        name="layer",
    )(*args)


def solution(mesh):
    in_specs = (
        P(("dp", "mp"), None, None),
        P(),
        P(("dp", "mp"), None),
        P(),
        P(),
        P(),
        P(),
        P(None, None, "dp", "mp"),
        P(None, None, "mp"),
        P(None, "mp", "dp"),
        P(),
        P(None, "dp", "mp"),
        P(None, "mp"),
        P(None, "mp", "dp"),
        P(),
    )
    return jax.shard_map(
        per_device,
        mesh=mesh,
        in_specs=in_specs,
        out_specs=P(("dp", "mp"), None),
        check_vma=False,
    )
```

```python
import jax
import jax.numpy as jnp
from jax import lax
from jax.experimental import pallas as pl
from jax.experimental.pallas import tpu as pltpu
from jax.sharding import PartitionSpec as P

BF = jnp.bfloat16
F32 = jnp.float32
MESH = pl.DeviceIdType.MESH
ALL = slice(None)
D = 1280
HEAD = 80
SLOT = 80
ROWS = 160
KEEP = 64
SCALE = 1.0 / HEAD**0.5

ORDERS = ("xyz", "yzx", "zxy")
SECTIONS = (
    ((0, 256), (640, 256), (1280, 128)),
    ((256, 256), (896, 128), (1408, 256)),
    ((512, 128), (1024, 256), (1664, 256)),
)
LANES = 1920
N_SEM = 124


def place():
    dp, mp = lax.axis_index("dp"), lax.axis_index("mp")
    return {
        "x": lax.rem(dp // 2, 2) * 2 + mp // 4,
        "y": lax.rem(mp, 4),
        "z": dp // 4,
        "c": lax.rem(dp, 2),
    }


def device(p):
    return (p["z"] * 4 + (p["x"] // 2) * 2 + p["c"], lax.rem(p["x"], 2) * 4 + p["y"])


def shifted(p, dim, by):
    return {**p, dim: lax.rem(p[dim] + by + 4, 4)}


def other_core(p):
    return {**p, "c": 1 - p["c"]}


def slab(colour, phase, p, half=None):
    free = ORDERS[colour][: phase - 1]
    at = {"xl": lax.rem(p["x"], 2), "xh": p["x"] // 2, "y": p["y"], "z": p["z"], "r": ALL}
    for dim in free:
        for part in ("xl", "xh") if dim == "x" else (dim,):
            at[part] = ALL
    if half is not None:
        if phase == 1:
            at["r"] = pl.ds(0, 48) if half == 0 else pl.ds(48, 32)
        else:
            part, count = ("xl", 1) if free[0] == "x" else (free[0], 2)
            at[part] = pl.ds(half * count, count)
    return (at["xl"], at["y"], at["z"], at["xh"], p["c"], at["r"])


class Transfer:
    def __init__(self, owner, sent, received, lanes, target):
        number = owner.count
        owner.count += 1
        self.owner = owner

        def copy(where):
            ref = owner.ref.at[where + (pl.ds(*lanes),)]
            return pltpu.make_async_remote_copy(
                src_ref=ref,
                dst_ref=ref,
                send_sem=owner.send.at[number],
                recv_sem=owner.recv.at[number],
                device_id=device(target),
                device_id_type=MESH,
            )

        self.out, self.into = copy(sent), copy(received)

    def start(self):
        self.out.start()
        self.owner.started.append(self.out)

    def wait(self):
        self.into.wait_recv()


class Gather:
    def __init__(self, p, ref, send, recv):
        self.p, self.ref, self.send, self.recv = p, ref, send, recv
        self.count, self.started = 0, []
        mate = other_core(p)
        self.own = Transfer(self, slab(0, 1, p), slab(0, 1, mate), (0, LANES), mate)
        self.first = [self.phase(k, 1, (640 * k, 640)) for k in range(3)]
        self.second = [self.phase(k, 2, (640 * k, 640)) for k in range(3)]
        self.third = [[self.phase(k, 3, s[k]) for k in range(3)] for s in SECTIONS]

    def phase(self, k, number, lanes):
        p = self.p
        dim = ORDERS[k][number - 1]
        up, down, far = shifted(p, dim, 1), shifted(p, dim, -1), shifted(p, dim, 2)
        mate = other_core(p)

        def at(q, half=None):
            return slab(k, number, q, half)

        def copy(sent, received, target):
            return Transfer(self, sent, received, lanes, target)

        return {
            "full_up": copy(at(p), at(down), up),
            "full_down": copy(at(p), at(up), down),
            "half_up": copy(at(down, 0), at(far, 0), up),
            "half_down": copy(at(up, 1), at(far, 1), down),
            "mate_down": copy(at(down), at(other_core(down)), mate),
            "mate_up": copy(at(up), at(other_core(up)), mate),
            "mate_far0": copy(at(far, 0), at(other_core(far), 0), mate),
            "mate_far1": copy(at(far, 1), at(other_core(far), 1), mate),
        }

    def fulls(self, group):
        for f in group:
            f["full_up"].start()
            f["full_down"].start()

    def halves(self, group):
        for f in group:
            f["full_up"].wait()
            f["half_up"].start()
            f["full_down"].wait()
            f["half_down"].start()
        for f in group:
            f["mate_down"].start()
            f["mate_up"].start()

    def far(self, group):
        for f in group:
            f["half_up"].wait()
            f["half_down"].wait()

    def far_to_mate(self, group):
        for f in group:
            f["mate_far0"].start()
            f["mate_far1"].start()

    def from_mate(self, group):
        for f in group:
            for name in ("mate_down", "mate_up", "mate_far0", "mate_far1"):
                f[name].wait()


def norm(values, gain, shift):
    mean = jnp.mean(values, axis=-1, keepdims=True)
    centred = values - mean
    spread = jnp.mean(centred * centred, axis=-1, keepdims=True)
    return (centred * lax.rsqrt(spread + 1e-06) * gain + shift).astype(BF)


def dot(a, b, contract=((1,), (0,))):
    return lax.dot_general(a, b, (contract, ((), ())), preferred_element_type=F32)


NT = ((1,), (1,))
TN = ((0,), (0,))


def kernel(
    patches,
    position,
    keep,
    counts,
    offsets,
    ln_gain,
    ln_bias,
    w_qkv,
    b_qkv,
    w_o,
    b_o,
    w_up,
    b_up,
    w_down,
    b_down,
    out,
    w,
    pictures,
    places,
    tokens,
    arrived,
    chosen,
    spread,
    slots,
    stream,
    normed,
    residual,
    hidden,
    biases,
    send,
    recv,
    load,
    send1,
    recv1,
    send1e,
    recv1e,
    sendb,
    recvb,
    send2,
    recv2,
    send2e,
    recv2e,
    send3,
    recv3,
    send3e,
    recv3e,
):
    dp, mp = lax.axis_index("dp"), lax.axis_index("mp")
    p = place()
    mate = other_core(p)
    tail_owner = (lax.rem(dp, 8), lax.rem(dp + 4, 8))
    has_tail = (mp == tail_owner[0]) | (mp == tail_owner[1])

    arrived[:, :, 128:256] = jnp.zeros((8, 256, 128), BF)

    barrier = pltpu.get_barrier_semaphore()

    def greet(target):
        pl.semaphore_signal(barrier, inc=1, device_id=target, device_id_type=MESH)

    for q in [shifted(p, d, s) for d in "xyz" for s in (1, -1)] + [mate]:
        greet(device(q))
    for k in range(1, 8):
        greet((dp, lax.rem(mp + k, 8)))
    for k in range(1, 16):
        greet((lax.rem(dp + k, 16), mp))

    load_pictures = pltpu.make_async_copy(patches, pictures, load.at[0])
    load_places = pltpu.make_async_copy(position, places, load.at[1])
    load_pictures.start()
    load_places.start()

    xl, xh = lax.rem(p["x"], 2), p["x"] // 2
    mine = (xl, p["y"], p["z"], xh, p["c"], ALL)

    def put(lane, value):
        w[mine + (pl.ds(lane, value.shape[1]),)] = value.astype(BF)

    eye = (
        lax.broadcasted_iota(jnp.int32, (SLOT, SLOT), 0)
        == lax.broadcasted_iota(jnp.int32, (SLOT, SLOT), 1)
    ).astype(F32).astype(BF)
    out_t = dot(eye, w_o[0], NT)
    down_t = w_down[0]
    qkv = [w_qkv[0, t].astype(F32) for t in range(3)]
    put(0, qkv[0][:, :128])
    put(128, qkv[1][:, :128])
    put(640, qkv[2][:, :128])
    put(768, jnp.concatenate([v[:, 128:160] for v in qkv] + [out_t[:, 128:160]], axis=1))
    put(1280, out_t[:, :128])
    put(256, w_up[0, :, 0:256])
    put(896, w_up[0, :, 256:384])
    put(1408, w_up[0, :, 384:640])
    put(512, down_t[:, 0:128])
    put(1024, down_t[:, 128:384])
    put(1664, down_t[:, 384:640])

    for t in range(3):
        biases[mp, t : t + 1, :] = b_qkv[t, 0:1, 0:128]
    biases[mp, 3:4, :] = jnp.concatenate(
        [b_qkv[t, 0:1, 128:160] for t in range(3)] + [jnp.zeros((1, 32), F32)], axis=1
    )
    for t in range(5):
        biases[mp, 4 + t : 5 + t, :] = b_up[0:1, t * 128 : (t + 1) * 128]

    pl.semaphore_wait(barrier, 29)

    g = Gather(p, w, send, recv)
    g.fulls(g.first)
    g.own.start()

    load_pictures.wait()
    load_places.wait()
    for i in range(4):
        hit = lax.broadcasted_iota(jnp.int32, (256, KEEP), 0) == keep[i : i + 1, :]
        hit = hit.astype(F32).astype(BF)
        picked = dot(hit, pictures[i], TN) + dot(hit, places[...], TN)
        tokens[i * KEEP : (i + 1) * KEEP, :] = picked.astype(BF)

    def tile(k):
        return pl.ds(pl.multiple_of(k * 128, 128), 128)

    first_sends = []
    for k in range(1, 8):
        peer = lax.rem(mp + k, 8)
        for src, dst, s, r in (
            (tokens.at[:, tile(peer)], arrived.at[mp, :, pl.ds(0, 128)], send1, recv1),
            (biases.at[mp], biases.at[mp], sendb, recvb),
        ):
            copy = pltpu.make_async_remote_copy(
                src_ref=src,
                dst_ref=dst,
                send_sem=s.at[k],
                recv_sem=r.at[mp],
                device_id=(dp, peer),
                device_id_type=MESH,
            )
            copy.start()
            first_sends.append(copy)
    tail_sends = []
    for k in range(2):
        copy = pltpu.make_async_remote_copy(
            src_ref=tokens.at[:, pl.ds(1024 + 128 * k, 128)],
            dst_ref=arrived.at[mp, :, pl.ds(128, 128)],
            send_sem=send1e.at[k],
            recv_sem=recv1e.at[mp],
            device_id=(dp, tail_owner[k]),
            device_id_type=MESH,
        )
        tail_sends.append(copy)

        @pl.when(mp != tail_owner[k])
        def _():
            copy.start()

        @pl.when(mp == tail_owner[k])
        def _():
            arrived[mp, :, 128:256] = tokens[:, 1024 + 128 * k : 1152 + 128 * k]

    arrived[mp, :, 0:128] = tokens[:, tile(mp)]

    lane = lax.broadcasted_iota(jnp.int32, (16, 128), 1)
    inner = jnp.where(lane < KEEP, lane, lane - KEEP)
    pieces = []
    for k in range(16):
        a, b = dp * 32 + 2 * k, dp * 32 + 2 * k + 1
        count = jnp.where(lane < KEEP, counts[a], counts[b])
        start = jnp.where(lane < KEEP, offsets[a], offsets[b])
        pieces.append(jnp.where(inner < count, start + inner, -1))
    goal = jnp.concatenate(pieces, axis=1)
    sub = lax.broadcasted_iota(jnp.int32, (16, 2048), 0)

    def choose(i, carry):
        shard = i // 5
        row = shard * 1280 + dp * SLOT + (i - shard * 5) * 16
        hit = (goal - row) == sub
        chosen[pl.ds(pl.multiple_of(i * 16, 16), 16), :] = hit.astype(F32).astype(BF)
        return carry

    lax.fori_loop(0, 40, choose, 0)
    g.halves(g.first)
    lax.fori_loop(40, 80, choose, 0)

    labels_row, labels_col = [], []
    for h in range(2):
        first = dp * 1280 + (mp * 2 + h) * SLOT
        down = first + lax.broadcasted_iota(jnp.int32, (SLOT, 128), 0)
        across = first + lax.broadcasted_iota(jnp.int32, (SLOT, 128), 1)

        def mark(i, carry):
            image = (mp * 2 + h) * 32 + i
            low = offsets[image]
            high = low + counts[image]
            return tuple(
                jnp.where((rows >= low) & (rows < high), i + 1, old)
                for rows, old in zip((down, across), carry)
            )

        zero = jnp.zeros((SLOT, 128), jnp.int32)
        col, row = lax.fori_loop(0, 32, mark, (zero, zero))
        labels_col.append(col)
        labels_row.append(row)
    same = [(labels_col[h] == labels_row[h])[:, :SLOT] for h in range(2)]
    used = jnp.concatenate([labels_col[h][:, 0:1] for h in range(2)], axis=0) > 0

    g.far(g.first)
    g.fulls(g.second)
    g.far_to_mate(g.first)

    def wait_first(ref, sem, source):
        pltpu.make_async_remote_copy(
            src_ref=ref,
            dst_ref=ref,
            send_sem=send1.at[0],
            recv_sem=sem.at[source],
            device_id=(dp, source),
            device_id_type=MESH,
        ).wait_recv()

    for k in range(1, 8):
        source = lax.rem(mp + k, 8)
        wait_first(arrived.at[source, :, pl.ds(0, 128)], recv1, source)

    @pl.when(has_tail)
    def _():
        for k in range(1, 8):
            source = lax.rem(mp + k, 8)
            wait_first(arrived.at[source, :, pl.ds(128, 128)], recv1e, source)

    group = arrived[...].reshape(2048, 256)
    for k in range(4):
        rows = pl.ds(k * 320, 320)
        spread[rows, :] = dot(chosen[rows, :], group).astype(BF)

    g.halves(g.second)

    def slot_rows(k):
        return pl.ds(pl.multiple_of(k * SLOT, 16), SLOT)

    second_sends = []
    for k in range(1, 16):
        shard = lax.rem(dp + k, 16)
        for extra in range(2):
            copy = pltpu.make_async_remote_copy(
                src_ref=spread.at[slot_rows(shard), pl.ds(128 * extra, 128)],
                dst_ref=slots.at[dp, :, pl.ds(128 * extra, 128)],
                send_sem=(send2e if extra else send2).at[k],
                recv_sem=(recv2e if extra else recv2).at[dp],
                device_id=(shard, mp),
                device_id_type=MESH,
            )
            if extra:
                pl.when(has_tail)(copy.start)
            else:
                copy.start()
            second_sends.append((copy, has_tail if extra else None))
    slots[dp] = spread[slot_rows(dp), :]

    g.far(g.second)
    g.fulls(g.third[0])
    g.fulls(g.third[1])
    g.far_to_mate(g.second)

    def wait_copy(ref, sem):
        pltpu.make_async_remote_copy(
            src_ref=ref,
            dst_ref=ref,
            send_sem=send1.at[0],
            recv_sem=sem,
            device_id=device(mate),
            device_id_type=MESH,
        ).wait_recv()

    for k in range(1, 16):
        source = lax.rem(dp + k, 16)
        wait_copy(slots.at[source, :, pl.ds(0, 128)], recv2.at[source])
    third_sends = []
    for k in range(1, 8):
        peer = lax.rem(mp + k, 8)
        copy = pltpu.make_async_remote_copy(
            src_ref=slots.at[pl.ds(peer * 2, 2), :, pl.ds(0, 128)],
            dst_ref=stream.at[:, :, tile(mp)],
            send_sem=send3.at[k],
            recv_sem=recv3.at[mp],
            device_id=(dp, peer),
            device_id_type=MESH,
        )
        copy.start()
        third_sends.append((copy, None))
    stream[:, :, tile(mp)] = slots[pl.ds(mp * 2, 2), :, 0:128]
    for k in range(4):
        source = lax.rem(mp + 4 * k, 16)
        place_tail = pl.ds(1024 + 128 * (k % 2), 128)

        @pl.when(source != dp)
        def _():
            wait_copy(slots.at[source, :, pl.ds(128, 128)], recv2e.at[source])

        copy = pltpu.make_async_remote_copy(
            src_ref=slots.at[source, :, pl.ds(128, 128)],
            dst_ref=stream.at[lax.rem(source, 2), :, place_tail],
            send_sem=send3e.at[k],
            recv_sem=recv3e.at[lax.rem(source, 2), k % 2],
            device_id=(dp, source // 2),
            device_id_type=MESH,
        )
        away = source // 2 != mp
        pl.when(away)(copy.start)
        third_sends.append((copy, away))

        @pl.when(jnp.logical_not(away))
        def _():
            stream[lax.rem(source, 2), :, place_tail] = slots[source, :, 128:256]

    g.halves(g.third[0])
    g.fulls(g.third[2])

    for k in range(1, 8):
        source = lax.rem(mp + k, 8)
        wait_copy(stream.at[:, :, tile(source)], recv3.at[source])
        wait_copy(biases.at[source], recvb.at[source])
    for h in range(2):
        for t in range(2):

            @pl.when(lax.rem(mp * 2 + h + 4 * t, 8) != mp)
            def _():
                wait_copy(stream.at[h, :, pl.ds(1024 + 128 * t, 128)], recv3e.at[h, t])

    rows_in = stream[...].reshape(ROWS, D).astype(F32)
    normed[...] = norm(rows_in, ln_gain[0, 0:1, :], ln_bias[0, 0:1, :])
    residual[...] = rows_in + b_o[...]

    g.halves(g.third[1])
    g.far(g.third[0])
    g.far_to_mate(g.third[0])
    g.own.wait()
    g.from_mate(g.first)
    g.from_mate(g.second)
    g.from_mate(g.third[0])

    def weights(m, *lanes):
        parts = [w[m // 4, lax.rem(m, 4), :, :, :, :, pl.ds(*v)].reshape(D, v[1]) for v in lanes]
        return parts[0] if len(parts) == 1 else jnp.concatenate(parts, axis=1)

    def attention(m, carry):
        rows = normed[...]
        bias = biases[m]

        def projected(lanes, t):
            both = dot(rows, weights(m, lanes))
            return [both[:, 128 * i : 128 * (i + 1)] + bias[t + i : t + i + 1, :] for i in range(2)]

        q, k = projected((0, 256), 0)
        v, tail = projected((640, 256), 2)
        heads = []
        for i, value in enumerate((q, k, v)):
            second = jnp.concatenate([value[:, 80:128], tail[:, 32 * i : 32 * i + 32]], axis=1)
            heads.append((value[:, :80].astype(BF), second.astype(BF)))
        mixed = []
        for n in range(2):
            blocks = []
            for h in range(2):
                part = slice(h * SLOT, (h + 1) * SLOT)
                scores = dot(heads[0][n][part], heads[1][n][part], NT) * SCALE
                scores = jnp.where(same[h], scores, -jnp.inf)
                raised = jnp.exp(scores - jnp.max(scores, axis=-1, keepdims=True))
                share = (raised / jnp.sum(raised, axis=-1, keepdims=True)).astype(BF)
                blocks.append(dot(share, heads[2][n][part]))
            mixed.append(jnp.concatenate(blocks, axis=0))
        left = jnp.concatenate([mixed[0], mixed[1][:, :48]], axis=1).astype(BF)
        right = jnp.concatenate([jnp.zeros((ROWS, 96), F32), mixed[1][:, 48:]], axis=1).astype(BF)
        both = jnp.concatenate([left, right], axis=1)
        residual[...] += dot(both, weights(m, (1280, 128), (768, 128)), NT)
        return carry

    lax.fori_loop(0, 8, attention, 0)
    normed[...] = norm(residual[...], ln_gain[0, 1:2, :], ln_bias[0, 1:2, :])
    residual[...] += b_down[...]

    g.halves(g.third[2])
    g.far(g.third[1])
    g.far_to_mate(g.third[1])
    g.from_mate(g.third[1])

    def up(m, carry):
        rows = normed[...]
        bias = biases[m]
        for lanes, first in (((256, 256), 0), ((896, 128), 2), ((1408, 256), 3)):
            value = dot(rows, weights(m, lanes))
            row = jnp.concatenate(
                [bias[4 + first + i : 5 + first + i, :] for i in range(lanes[1] // 128)], axis=1
            )
            value = value + row
            value = 0.5 * value * (1.0 + lax.erf(value * (0.5**0.5)))
            hidden[m, :, first * 128 : first * 128 + lanes[1]] = value.astype(BF)
        return carry

    lax.fori_loop(0, 8, up, 0)

    g.far(g.third[2])
    g.far_to_mate(g.third[2])
    g.from_mate(g.third[2])

    def down(m, carry):
        residual[...] += dot(
            hidden[m], weights(m, (512, 128), (1024, 256), (1664, 256)), NT
        )
        return carry

    lax.fori_loop(0, 8, down, 0)
    out[...] = jnp.where(used, residual[...], 0.0).astype(BF)

    for copy in g.started + first_sends:
        copy.wait_send()
    for k in range(2):
        pl.when(mp != tail_owner[k])(tail_sends[k].wait_send)
    for copy, away in second_sends + third_sends:
        if away is None:
            copy.wait_send()
        else:
            pl.when(away)(copy.wait_send)


def per_device(*args):
    args = list(args)
    args[8] = jnp.transpose(args[8], (1, 0, 2))
    args[13] = jnp.transpose(args[13], (0, 2, 1))
    vmem = pl.BlockSpec(memory_space=pltpu.VMEM)
    smem = pl.BlockSpec(memory_space=pltpu.SMEM)
    anywhere = pl.BlockSpec(memory_space=pl.ANY)
    specs = [anywhere, anywhere, vmem, smem, smem] + [vmem] * 10
    dma = pltpu.SemaphoreType.DMA
    return pl.pallas_call(
        kernel,
        out_shape=jax.ShapeDtypeStruct((ROWS, D), BF),
        in_specs=specs,
        out_specs=vmem,
        scratch_shapes=[
            pltpu.VMEM((2, 4, 4, 2, 2, SLOT, LANES), BF),
            pltpu.VMEM((4, 256, D), BF),
            pltpu.VMEM((256, D), BF),
            pltpu.VMEM((256, D), BF),
            pltpu.VMEM((8, 256, 256), BF),
            pltpu.VMEM((1280, 2048), BF),
            pltpu.VMEM((1280, 256), BF),
            pltpu.VMEM((16, SLOT, 256), BF),
            pltpu.VMEM((2, SLOT, D), BF),
            pltpu.VMEM((ROWS, D), BF),
            pltpu.VMEM((ROWS, D), F32),
            pltpu.VMEM((8, ROWS, 640), BF),
            pltpu.VMEM((8, 16, 128), F32),
            dma((N_SEM,)),
            dma((N_SEM,)),
            dma((2,)),
            dma((8,)),
            dma((8,)),
            dma((2,)),
            dma((8,)),
            dma((8,)),
            dma((8,)),
            dma((16,)),
            dma((16,)),
            dma((16,)),
            dma((16,)),
            dma((8,)),
            dma((8,)),
            dma((4,)),
            dma((2, 2)),
        ],
        compiler_params=pltpu.CompilerParams(
            collective_id=0, has_side_effects=True, vmem_limit_bytes=62 * 1024 * 1024
        ),
        name="layer",
    )(*args)


def solution(mesh):
    in_specs = (
        P(("dp", "mp"), None, None),
        P(),
        P(("dp", "mp"), None),
        P(),
        P(),
        P(),
        P(),
        P(None, None, "dp", "mp"),
        P(None, None, "mp"),
        P(None, "mp", "dp"),
        P(),
        P(None, "dp", "mp"),
        P(None, "mp"),
        P(None, "mp", "dp"),
        P(),
    )
    return jax.shard_map(
        per_device,
        mesh=mesh,
        in_specs=in_specs,
        out_specs=P(("dp", "mp"), None),
        check_vma=False,
    )
```

```python
import jax
import jax.numpy as jnp
from jax import lax
from jax.experimental import pallas as pl
from jax.experimental.pallas import tpu as pltpu
from jax.sharding import PartitionSpec as P

BF = jnp.bfloat16
F32 = jnp.float32
MESH = pl.DeviceIdType.MESH
ALL = slice(None)
D = 1280
HEAD = 80
SLOT = 80
ROWS = 160
KEEP = 64
SCALE = 1.0 / HEAD**0.5

ORDERS = ("xyz", "yzx", "zxy")
COLOURS = ((0, 256), (256, 256), (512, 128))
Q_K, V_TAIL, OUT, TAIL = (0, 256), (256, 256), (512, 128), (384, 128)
PLANES = ("yz", "zy")
RING = ((0, 640), (640, 640))
UP = ((0, 256), (640, 384))
DOWN = ((256, 384), (1024, 256))
N_SEM = 116
N_MLP = 82
PIECES = (0, -1, 1, 2)
FORWARD = {1: (0, -1), -1: (1, 2)}
FORWARD_TWO = {1: (0,), -1: (1,)}


def place():
    dp, mp = lax.axis_index("dp"), lax.axis_index("mp")
    return {
        "x": lax.rem(dp // 2, 2) * 2 + mp // 4,
        "y": lax.rem(mp, 4),
        "z": dp // 4,
        "c": lax.rem(dp, 2),
    }


def device(p):
    return (p["z"] * 4 + (p["x"] // 2) * 2 + p["c"], lax.rem(p["x"], 2) * 4 + p["y"])


def shifted(p, dim, by):
    return {**p, dim: lax.rem(p[dim] + by + 4, 4)}


def other_core(p):
    return {**p, "c": 1 - p["c"]}


def slab(colour, phase, p, half=None):
    free = ORDERS[colour][: phase - 1]
    at = {"xl": lax.rem(p["x"], 2), "xh": p["x"] // 2, "y": p["y"], "z": p["z"], "r": ALL}
    for dim in free:
        for part in ("xl", "xh") if dim == "x" else (dim,):
            at[part] = ALL
    if half is not None:
        at["r"] = pl.ds(0, 48) if half == 0 else pl.ds(48, 32)
    return (at["xl"], at["y"], at["z"], at["xh"], p["c"], at["r"])


class Transfer:
    def __init__(self, owner, sent, received, lanes, target):
        number = owner.count
        owner.count += 1
        self.owner = owner

        def copy(where):
            ref = owner.ref.at[where + (pl.ds(*lanes),)]
            return pltpu.make_async_remote_copy(
                src_ref=ref,
                dst_ref=ref,
                send_sem=owner.send.at[number],
                recv_sem=owner.recv.at[number],
                device_id=device(target),
                device_id_type=MESH,
            )

        self.out, self.into = copy(sent), copy(received)

    def start(self):
        self.out.start()
        self.owner.started.append(self.out)

    def wait(self):
        self.into.wait_recv()


class Gather:
    def __init__(self, p, ref, send, recv):
        self.p, self.ref, self.send, self.recv = p, ref, send, recv
        self.count, self.started = 0, []

    def cross(self, piece, whole, dim, lanes, pieces, forward):
        p, mate = self.p, other_core(self.p)
        out = {"forward": forward}
        for way in (1, -1):
            target, source, far = shifted(p, dim, way), shifted(p, dim, -way), shifted(p, dim, 2)
            for r in pieces:
                out["full", way, r] = Transfer(self, piece(p, r), piece(source, r), lanes, target)
            for r in forward[way]:
                out["half", way, r] = Transfer(self, piece(source, r), piece(far, r), lanes, target)
        for way in (1, -1, 2):
            q = shifted(p, dim, way)
            out["mate", way] = Transfer(self, whole(q), whole(other_core(q)), lanes, mate)
        return out

    def offer(self, group, pieces):
        for r in pieces:
            for f in group:
                for way in (1, -1):
                    f["full", way, r].start()

    def relay(self, group, pieces):
        for r in pieces:
            for f in group:
                for way in (1, -1):
                    f["full", way, r].wait()
                    if r in f["forward"][way]:
                        f["half", way, r].start()

    def to_mate(self, group):
        for f in group:
            for way in (1, -1):
                f["mate", way].start()

    def last(self, group):
        for f in group:
            for way in (1, -1):
                for r in f["forward"][way]:
                    f["half", way, r].wait()

    def last_to_mate(self, group):
        for f in group:
            f["mate", 2].start()

    def all_from_mate(self, group):
        for f in group:
            for way in (1, -1, 2):
                f["mate", way].wait()

    def fulls(self, group):
        for f in group:
            f["full_up"].start()
            f["full_down"].start()

    def halves(self, group):
        for f in group:
            f["full_up"].wait()
            f["half_up"].start()
            f["full_down"].wait()
            f["half_down"].start()
        for f in group:
            f["mate_down"].start()
            f["mate_up"].start()

    def far(self, group):
        for f in group:
            f["half_up"].wait()
            f["half_down"].wait()

    def far_to_mate(self, group):
        for f in group:
            f["mate_far0"].start()
            f["mate_far1"].start()

    def from_mate(self, group):
        for f in group:
            for name in ("mate_down", "mate_up", "mate_far0", "mate_far1"):
                f[name].wait()


class Attention(Gather):
    def __init__(self, p, ref, send, recv):
        super().__init__(p, ref, send, recv)
        mate = other_core(p)
        self.own = Transfer(self, slab(0, 1, p), slab(0, 1, mate), (0, 640), mate)
        self.first = [self.ring(k, COLOURS[k]) for k in range(3)]
        self.second = [self.span(k, 2, COLOURS[k]) for k in range(3)]
        self.third = [self.span(k, 3, COLOURS[k]) for k in range(3)]

    def span(self, k, number, lanes):
        inner, dim = ORDERS[k][number - 2], ORDERS[k][number - 1]
        return self.cross(
            lambda q, r: slab(k, number - 1, shifted(q, inner, r)),
            lambda q: slab(k, number, q),
            dim,
            lanes,
            PIECES,
            FORWARD,
        )

    def ring(self, k, lanes):
        p = self.p
        dim = ORDERS[k][0]
        up, down, far = shifted(p, dim, 1), shifted(p, dim, -1), shifted(p, dim, 2)
        mate = other_core(p)

        def at(q, half=None):
            return slab(k, 1, q, half)

        def copy(sent, received, target):
            return Transfer(self, sent, received, lanes, target)

        return {
            "full_up": copy(at(p), at(down), up),
            "full_down": copy(at(p), at(up), down),
            "half_up": copy(at(down, 0), at(far, 0), up),
            "half_down": copy(at(up, 1), at(far, 1), down),
            "mate_down": copy(at(down), at(other_core(down)), mate),
            "mate_up": copy(at(up), at(other_core(up)), mate),
            "mate_far0": copy(at(far, 0), at(other_core(far), 0), mate),
            "mate_far1": copy(at(far, 1), at(other_core(far), 1), mate),
        }


class Mlp(Gather):
    def __init__(self, p, ref, send, recv):
        super().__init__(p, ref, send, recv)
        mate, over = other_core(p), shifted(p, "x", 2)
        whole = (0, 1280)
        self.own = Transfer(self, self.at(p), self.at(mate), whole, mate)
        self.over = Transfer(self, self.at(p), self.at(over), whole, over)
        self.over_mate = Transfer(self, self.at(over), self.at(other_core(over)), whole, mate)
        self.ring = [
            self.cross(
                lambda q, r: self.at(shifted(q, "x", 2 * r)),
                lambda q: self.at(q, "x"),
                PLANES[k][0],
                RING[k],
                (0, 1),
                FORWARD_TWO,
            )
            for k in range(2)
        ]
        self.up = [self.span(k, UP[k]) for k in range(2)]
        self.down = [self.span(k, DOWN[k]) for k in range(2)]

    def at(self, q, free=""):
        return (
            ALL if "y" in free else q["y"],
            ALL if "z" in free else q["z"],
            ALL if "x" in free else q["x"] // 2,
            q["c"],
            ALL,
        )

    def span(self, k, lanes):
        inner, dim = PLANES[k]
        return self.cross(
            lambda q, r: self.at(shifted(q, inner, r), "x"),
            lambda q: self.at(q, "x" + inner),
            dim,
            lanes,
            PIECES,
            FORWARD,
        )


def norm(values, gain, shift):
    mean = jnp.mean(values, axis=-1, keepdims=True)
    centred = values - mean
    spread = jnp.mean(centred * centred, axis=-1, keepdims=True)
    return (centred * lax.rsqrt(spread + 1e-06) * gain + shift).astype(BF)


def dot(a, b, contract=((1,), (0,))):
    return lax.dot_general(a, b, (contract, ((), ())), preferred_element_type=F32)


NT = ((1,), (1,))
TN = ((0,), (0,))


def kernel(
    patches,
    position,
    keep,
    counts,
    offsets,
    ln_gain,
    ln_bias,
    w_qkv,
    b_qkv,
    w_o,
    b_o,
    w_up,
    b_up,
    w_down,
    b_down,
    out,
    w,
    w_mlp,
    pictures,
    places,
    tokens,
    arrived,
    chosen,
    spread,
    slots,
    stream,
    normed,
    pair_rows,
    residual,
    hidden,
    partial,
    returned,
    biases,
    send,
    recv,
    send_mlp,
    recv_mlp,
    send_pair,
    recv_pair,
    load,
    send1,
    recv1,
    send1e,
    recv1e,
    sendb,
    recvb,
    send2,
    recv2,
    send2e,
    recv2e,
    send3,
    recv3,
    send3e,
    recv3e,
):
    dp, mp = lax.axis_index("dp"), lax.axis_index("mp")
    p = place()
    mate = other_core(p)
    tail_owner = (lax.rem(dp, 8), lax.rem(dp + 4, 8))
    has_tail = (mp == tail_owner[0]) | (mp == tail_owner[1])

    arrived[:, :, 128:256] = jnp.zeros((8, 256, 128), BF)

    barrier = pltpu.get_barrier_semaphore()

    def greet(target):
        pl.semaphore_signal(barrier, inc=1, device_id=target, device_id_type=MESH)

    for q in [shifted(p, d, s) for d in "xyz" for s in (1, -1)] + [mate]:
        greet(device(q))
    for k in range(1, 8):
        greet((dp, lax.rem(mp + k, 8)))
    for k in range(1, 16):
        greet((lax.rem(dp + k, 16), mp))

    load_pictures = pltpu.make_async_copy(patches, pictures, load.at[0])
    load_places = pltpu.make_async_copy(position, places, load.at[1])
    load_pictures.start()
    load_places.start()

    xl, xh = lax.rem(p["x"], 2), p["x"] // 2
    mine = (xl, p["y"], p["z"], xh, p["c"], ALL)

    def put(lane, value):
        w[mine + (pl.ds(lane, value.shape[1]),)] = value.astype(BF)

    def put_mlp(lane, value):
        w_mlp[mine[1:] + (pl.ds(lane, value.shape[1]),)] = value

    eye = (
        lax.broadcasted_iota(jnp.int32, (SLOT, SLOT), 0)
        == lax.broadcasted_iota(jnp.int32, (SLOT, SLOT), 1)
    ).astype(F32).astype(BF)
    out_t = dot(eye, w_o[0], NT)
    qkv = [w_qkv[0, t].astype(F32) for t in range(3)]
    put(0, qkv[0][:, :128])
    put(128, qkv[1][:, :128])
    put(256, qkv[2][:, :128])
    put(384, jnp.concatenate([v[:, 128:160] for v in qkv] + [out_t[:, 128:160]], axis=1))
    put(512, out_t[:, :128])
    put_mlp(0, w_up[0, :, 0:256])
    put_mlp(640, w_up[0, :, 256:640])
    put_mlp(256, w_down[0, :, 0:384])
    put_mlp(1024, w_down[0, :, 384:640])

    for t in range(3):
        biases[mp, t : t + 1, :] = b_qkv[t, 0:1, 0:128]
    biases[mp, 3:4, :] = jnp.concatenate(
        [b_qkv[t, 0:1, 128:160] for t in range(3)] + [jnp.zeros((1, 32), F32)], axis=1
    )
    for t in range(5):
        biases[mp, 4 + t : 5 + t, :] = b_up[0:1, t * 128 : (t + 1) * 128]

    pl.semaphore_wait(barrier, 29)

    g = Attention(p, w, send, recv)
    mlp = Mlp(p, w_mlp, send_mlp, recv_mlp)
    g.fulls(g.first)
    mlp.over.start()
    g.offer(g.second, (0,))
    mlp.offer(mlp.ring, (0,))
    g.own.start()
    mlp.own.start()

    load_pictures.wait()
    load_places.wait()
    for i in range(4):
        hit = lax.broadcasted_iota(jnp.int32, (256, KEEP), 0) == keep[i : i + 1, :]
        hit = hit.astype(F32).astype(BF)
        picked = dot(hit, pictures[i], TN) + dot(hit, places[...], TN)
        tokens[i * KEEP : (i + 1) * KEEP, :] = picked.astype(BF)

    def tile(k):
        return pl.ds(pl.multiple_of(k * 128, 128), 128)

    first_sends = []
    for k in range(1, 8):
        peer = lax.rem(mp + k, 8)
        for src, dst, s, r in (
            (tokens.at[:, tile(peer)], arrived.at[mp, :, pl.ds(0, 128)], send1, recv1),
            (biases.at[mp], biases.at[mp], sendb, recvb),
        ):
            copy = pltpu.make_async_remote_copy(
                src_ref=src,
                dst_ref=dst,
                send_sem=s.at[k],
                recv_sem=r.at[mp],
                device_id=(dp, peer),
                device_id_type=MESH,
            )
            copy.start()
            first_sends.append(copy)
    tail_sends = []
    for k in range(2):
        copy = pltpu.make_async_remote_copy(
            src_ref=tokens.at[:, pl.ds(1024 + 128 * k, 128)],
            dst_ref=arrived.at[mp, :, pl.ds(128, 128)],
            send_sem=send1e.at[k],
            recv_sem=recv1e.at[mp],
            device_id=(dp, tail_owner[k]),
            device_id_type=MESH,
        )
        tail_sends.append(copy)

        @pl.when(mp != tail_owner[k])
        def _():
            copy.start()

        @pl.when(mp == tail_owner[k])
        def _():
            arrived[mp, :, 128:256] = tokens[:, 1024 + 128 * k : 1152 + 128 * k]

    arrived[mp, :, 0:128] = tokens[:, tile(mp)]

    lane = lax.broadcasted_iota(jnp.int32, (16, 128), 1)
    inner = jnp.where(lane < KEEP, lane, lane - KEEP)
    pieces = []
    for k in range(16):
        a, b = dp * 32 + 2 * k, dp * 32 + 2 * k + 1
        count = jnp.where(lane < KEEP, counts[a], counts[b])
        start = jnp.where(lane < KEEP, offsets[a], offsets[b])
        pieces.append(jnp.where(inner < count, start + inner, -1))
    goal = jnp.concatenate(pieces, axis=1)
    sub = lax.broadcasted_iota(jnp.int32, (16, 2048), 0)

    def choose(i, carry):
        shard = i // 5
        row = shard * 1280 + dp * SLOT + (i - shard * 5) * 16
        hit = (goal - row) == sub
        chosen[pl.ds(pl.multiple_of(i * 16, 16), 16), :] = hit.astype(F32).astype(BF)
        return carry

    lax.fori_loop(0, 40, choose, 0)
    g.halves(g.first)
    g.offer(g.second, (-1, 1))
    lax.fori_loop(40, 80, choose, 0)

    labels_row, labels_col = [], []
    for h in range(2):
        first = dp * 1280 + (mp * 2 + h) * SLOT
        down = first + lax.broadcasted_iota(jnp.int32, (SLOT, 128), 0)
        across = first + lax.broadcasted_iota(jnp.int32, (SLOT, 128), 1)

        def mark(i, carry):
            image = (mp * 2 + h) * 32 + i
            low = offsets[image]
            high = low + counts[image]
            return tuple(
                jnp.where((rows >= low) & (rows < high), i + 1, old)
                for rows, old in zip((down, across), carry)
            )

        zero = jnp.zeros((SLOT, 128), jnp.int32)
        col, row = lax.fori_loop(0, 32, mark, (zero, zero))
        labels_col.append(col)
        labels_row.append(row)
    same = [(labels_col[h] == labels_row[h])[:, :SLOT] for h in range(2)]
    used = jnp.concatenate([labels_col[h][:, 0:1] for h in range(2)], axis=0) > 0

    g.far(g.first)
    g.offer(g.second, (2,))
    g.offer(g.third, (0,))
    g.far_to_mate(g.first)

    g.relay(g.second, (0, -1, 1))
    mlp.over.wait()
    mlp.offer(mlp.ring, (1,))
    mlp.over_mate.start()

    def wait_first(ref, sem, source):
        pltpu.make_async_remote_copy(
            src_ref=ref,
            dst_ref=ref,
            send_sem=send1.at[0],
            recv_sem=sem.at[source],
            device_id=(dp, source),
            device_id_type=MESH,
        ).wait_recv()

    for k in range(1, 8):
        source = lax.rem(mp + k, 8)
        wait_first(arrived.at[source, :, pl.ds(0, 128)], recv1, source)

    @pl.when(has_tail)
    def _():
        for k in range(1, 8):
            source = lax.rem(mp + k, 8)
            wait_first(arrived.at[source, :, pl.ds(128, 128)], recv1e, source)

    group = arrived[...].reshape(2048, 256)
    for k in range(4):
        rows = pl.ds(k * 320, 320)
        spread[rows, :] = dot(chosen[rows, :], group).astype(BF)

    def slot_rows(k):
        return pl.ds(pl.multiple_of(k * SLOT, 16), SLOT)

    second_sends = []
    for k in range(1, 16):
        shard = lax.rem(dp + k, 16)
        for extra in range(2):
            copy = pltpu.make_async_remote_copy(
                src_ref=spread.at[slot_rows(shard), pl.ds(128 * extra, 128)],
                dst_ref=slots.at[dp, :, pl.ds(128 * extra, 128)],
                send_sem=(send2e if extra else send2).at[k],
                recv_sem=(recv2e if extra else recv2).at[dp],
                device_id=(shard, mp),
                device_id_type=MESH,
            )
            if extra:
                pl.when(has_tail)(copy.start)
            else:
                copy.start()
            second_sends.append((copy, has_tail if extra else None))
    slots[dp] = spread[slot_rows(dp), :]

    g.relay(g.second, (2,))
    g.offer(g.third, (-1, 1))
    g.to_mate(g.second)
    g.last(g.second)
    g.offer(g.third, (2,))
    g.last_to_mate(g.second)

    mlp.relay(mlp.ring, (0, 1))
    mlp.to_mate(mlp.ring)
    mlp.offer(mlp.up, (0,))
    mlp.last(mlp.ring)
    mlp.last_to_mate(mlp.ring)

    def wait_copy(ref, sem):
        pltpu.make_async_remote_copy(
            src_ref=ref,
            dst_ref=ref,
            send_sem=send1.at[0],
            recv_sem=sem,
            device_id=device(mate),
            device_id_type=MESH,
        ).wait_recv()

    for k in range(1, 16):
        source = lax.rem(dp + k, 16)
        wait_copy(slots.at[source, :, pl.ds(0, 128)], recv2.at[source])
    third_sends = []
    for k in range(1, 8):
        peer = lax.rem(mp + k, 8)
        copy = pltpu.make_async_remote_copy(
            src_ref=slots.at[pl.ds(peer * 2, 2), :, pl.ds(0, 128)],
            dst_ref=stream.at[:, :, tile(mp)],
            send_sem=send3.at[k],
            recv_sem=recv3.at[mp],
            device_id=(dp, peer),
            device_id_type=MESH,
        )
        copy.start()
        third_sends.append((copy, None))
    stream[:, :, tile(mp)] = slots[pl.ds(mp * 2, 2), :, 0:128]
    for k in range(4):
        source = lax.rem(mp + 4 * k, 16)
        place_tail = pl.ds(1024 + 128 * (k % 2), 128)

        @pl.when(source != dp)
        def _():
            wait_copy(slots.at[source, :, pl.ds(128, 128)], recv2e.at[source])

        copy = pltpu.make_async_remote_copy(
            src_ref=slots.at[source, :, pl.ds(128, 128)],
            dst_ref=stream.at[lax.rem(source, 2), :, place_tail],
            send_sem=send3e.at[k],
            recv_sem=recv3e.at[lax.rem(source, 2), k % 2],
            device_id=(dp, source // 2),
            device_id_type=MESH,
        )
        away = source // 2 != mp
        pl.when(away)(copy.start)
        third_sends.append((copy, away))

        @pl.when(jnp.logical_not(away))
        def _():
            stream[lax.rem(source, 2), :, place_tail] = slots[source, :, 128:256]

    g.relay(g.third, PIECES)
    g.to_mate(g.third)
    mlp.offer(mlp.up, (-1, 1, 2))

    mlp.offer(mlp.down, PIECES)

    for k in range(1, 8):
        source = lax.rem(mp + k, 8)
        wait_copy(stream.at[:, :, tile(source)], recv3.at[source])
        wait_copy(biases.at[source], recvb.at[source])
    for h in range(2):
        for t in range(2):

            @pl.when(lax.rem(mp * 2 + h + 4 * t, 8) != mp)
            def _():
                wait_copy(stream.at[h, :, pl.ds(1024 + 128 * t, 128)], recv3e.at[h, t])

    rows_in = stream[...].reshape(ROWS, D).astype(F32)
    normed[...] = norm(rows_in, ln_gain[0, 0:1, :], ln_bias[0, 0:1, :])
    residual[...] = rows_in + b_o[...]

    g.last(g.third)
    g.last_to_mate(g.third)
    g.own.wait()
    g.from_mate(g.first)
    g.all_from_mate(g.second)
    g.all_from_mate(g.third)

    def weights(m, *lanes):
        parts = [w[m // 4, lax.rem(m, 4), :, :, :, :, pl.ds(*v)].reshape(D, v[1]) for v in lanes]
        return parts[0] if len(parts) == 1 else jnp.concatenate(parts, axis=1)

    def attention(m, carry):
        rows = normed[...]
        bias = biases[m]

        def projected(lanes, t):
            both = dot(rows, weights(m, lanes))
            return [both[:, 128 * i : 128 * (i + 1)] + bias[t + i : t + i + 1, :] for i in range(2)]

        q, k = projected(Q_K, 0)
        v, tail = projected(V_TAIL, 2)
        heads = []
        for i, value in enumerate((q, k, v)):
            second = jnp.concatenate([value[:, 80:128], tail[:, 32 * i : 32 * i + 32]], axis=1)
            heads.append((value[:, :80].astype(BF), second.astype(BF)))
        mixed = []
        for n in range(2):
            blocks = []
            for h in range(2):
                part = slice(h * SLOT, (h + 1) * SLOT)
                scores = dot(heads[0][n][part], heads[1][n][part], NT) * SCALE
                scores = jnp.where(same[h], scores, -jnp.inf)
                raised = jnp.exp(scores - jnp.max(scores, axis=-1, keepdims=True))
                share = (raised / jnp.sum(raised, axis=-1, keepdims=True)).astype(BF)
                blocks.append(dot(share, heads[2][n][part]))
            mixed.append(jnp.concatenate(blocks, axis=0))
        left = jnp.concatenate([mixed[0], mixed[1][:, :48]], axis=1).astype(BF)
        right = jnp.concatenate([jnp.zeros((ROWS, 96), F32), mixed[1][:, 48:]], axis=1).astype(BF)
        both = jnp.concatenate([left, right], axis=1)
        residual[...] += dot(both, weights(m, OUT, TAIL), NT)
        return carry

    lax.fori_loop(0, 4, attention, 0)
    mlp.relay(mlp.up, PIECES)
    mlp.to_mate(mlp.up)
    lax.fori_loop(4, 8, attention, 0)
    pair_rows[0:ROWS, :] = norm(residual[...], ln_gain[0, 1:2, :], ln_bias[0, 1:2, :])
    residual[...] += b_down[...]

    sides = (device(shifted(p, "x", 1)), device(shifted(p, "x", -1)))
    pair_sends = []

    def to_pair(src, dst, number, target):
        copy = pltpu.make_async_remote_copy(
            src_ref=src,
            dst_ref=dst,
            send_sem=send_pair.at[number],
            recv_sem=recv_pair.at[number],
            device_id=target,
            device_id_type=MESH,
        )
        copy.start()
        pair_sends.append(copy)

    for k in range(2):
        to_pair(
            pair_rows.at[pl.ds(SLOT * k, SLOT)],
            pair_rows.at[pl.ds(ROWS + SLOT * k, SLOT)],
            k,
            sides[k],
        )

    mlp.relay(mlp.down, PIECES)
    mlp.to_mate(mlp.down)
    mlp.last(mlp.up)
    mlp.last_to_mate(mlp.up)
    mlp.own.wait()
    mlp.over_mate.wait()
    mlp.all_from_mate(mlp.ring)
    mlp.all_from_mate(mlp.up)
    pair_sends[0].wait_recv()
    pair_sends[1].wait_recv()

    def up(y, carry):
        rows = pair_rows[...]
        bias = biases[xl * 4 + y]
        first = 0
        for lanes in UP:
            value = dot(rows, w_mlp[y, :, :, :, :, pl.ds(*lanes)].reshape(D, lanes[1]))
            tiles = lanes[1] // 128
            row = [bias[4 + first + i : 5 + first + i, :] for i in range(tiles)]
            value = value + jnp.concatenate(row, axis=1)
            value = 0.5 * value * (1.0 + lax.erf(value * (0.5**0.5)))
            hidden[y, :, first * 128 : (first + tiles) * 128] = value.astype(BF)
            first += tiles
        return carry

    lax.fori_loop(0, 4, up, 0)

    mlp.last(mlp.down)
    mlp.last_to_mate(mlp.down)
    mlp.all_from_mate(mlp.down)

    def down_weights(y, z, count):
        parts = [
            w_mlp[y, pl.ds(z, count), :, :, :, pl.ds(*v)].reshape(count * 320, v[1]) for v in DOWN
        ]
        return jnp.concatenate(parts, axis=1)

    for n in range(2):
        total = 0.0
        for y in range(4):
            total = total + dot(hidden[y, ROWS:, :], down_weights(y, 2 * n, 2), NT)
        columns = pl.ds(640 * n, 640)
        partial[:, columns] = total.astype(BF)
        for k in range(2):
            block = (pl.ds(SLOT * k, SLOT), columns)
            to_pair(partial.at[block], returned.at[block], 2 + 2 * n + k, sides[1 - k])

    def down(y, carry):
        residual[...] += dot(hidden[y, :ROWS, :], down_weights(y, 0, 4), NT)
        return carry

    lax.fori_loop(0, 4, down, 0)
    for n in range(4):
        pair_sends[2 + n].wait_recv()
    total = residual[...] + returned[...].astype(F32)
    out[...] = jnp.where(used, total, 0.0).astype(BF)

    for copy in g.started + mlp.started + first_sends + pair_sends:
        copy.wait_send()
    for k in range(2):
        pl.when(mp != tail_owner[k])(tail_sends[k].wait_send)
    for copy, away in second_sends + third_sends:
        if away is None:
            copy.wait_send()
        else:
            pl.when(away)(copy.wait_send)


def per_device(*args):
    args = list(args)
    args[8] = jnp.transpose(args[8], (1, 0, 2))
    args[13] = jnp.transpose(args[13], (0, 2, 1))
    vmem = pl.BlockSpec(memory_space=pltpu.VMEM)
    smem = pl.BlockSpec(memory_space=pltpu.SMEM)
    anywhere = pl.BlockSpec(memory_space=pl.ANY)
    specs = [anywhere, anywhere, vmem, smem, smem] + [vmem] * 10
    dma = pltpu.SemaphoreType.DMA
    return pl.pallas_call(
        kernel,
        out_shape=jax.ShapeDtypeStruct((ROWS, D), BF),
        in_specs=specs,
        out_specs=vmem,
        scratch_shapes=[
            pltpu.VMEM((2, 4, 4, 2, 2, SLOT, 640), BF),
            pltpu.VMEM((4, 4, 2, 2, SLOT, 1280), BF),
            pltpu.VMEM((4, 256, D), BF),
            pltpu.VMEM((256, D), BF),
            pltpu.VMEM((256, D), BF),
            pltpu.VMEM((8, 256, 256), BF),
            pltpu.VMEM((1280, 2048), BF),
            pltpu.VMEM((1280, 256), BF),
            pltpu.VMEM((16, SLOT, 256), BF),
            pltpu.VMEM((2, SLOT, D), BF),
            pltpu.VMEM((ROWS, D), BF),
            pltpu.VMEM((2 * ROWS, D), BF),
            pltpu.VMEM((ROWS, D), F32),
            pltpu.VMEM((4, 2 * ROWS, 640), BF),
            pltpu.VMEM((ROWS, D), BF),
            pltpu.VMEM((ROWS, D), BF),
            pltpu.VMEM((8, 16, 128), F32),
            dma((N_SEM,)),
            dma((N_SEM,)),
            dma((N_MLP,)),
            dma((N_MLP,)),
            dma((6,)),
            dma((6,)),
            dma((2,)),
            dma((8,)),
            dma((8,)),
            dma((2,)),
            dma((8,)),
            dma((8,)),
            dma((8,)),
            dma((16,)),
            dma((16,)),
            dma((16,)),
            dma((16,)),
            dma((8,)),
            dma((8,)),
            dma((4,)),
            dma((2, 2)),
        ],
        compiler_params=pltpu.CompilerParams(
            collective_id=0, has_side_effects=True, vmem_limit_bytes=62 * 1024 * 1024
        ),
        name="layer",
    )(*args)


def solution(mesh):
    in_specs = (
        P(("dp", "mp"), None, None),
        P(),
        P(("dp", "mp"), None),
        P(),
        P(),
        P(),
        P(),
        P(None, None, "dp", "mp"),
        P(None, None, "mp"),
        P(None, "mp", "dp"),
        P(),
        P(None, "dp", "mp"),
        P(None, "mp"),
        P(None, "mp", "dp"),
        P(),
    )
    return jax.shard_map(
        per_device,
        mesh=mesh,
        in_specs=in_specs,
        out_specs=P(("dp", "mp"), None),
        check_vma=False,
    )
```

```python
import jax
import jax.numpy as jnp
from jax import lax
from jax.experimental import pallas as pl
from jax.experimental.pallas import tpu as pltpu
from jax.sharding import PartitionSpec as P

BF = jnp.bfloat16
F32 = jnp.float32
MESH = pl.DeviceIdType.MESH
ALL = slice(None)
D = 1280
HEAD = 80
SLOT = 80
ROWS = 160
KEEP = 64
SCALE = 1.0 / HEAD**0.5

ORDERS = ("yxz", "zyx", "xzy")
COLOURS = ((0, 256), (256, 256), (512, 128))
Q_K, V_TAIL, OUT, TAIL = (0, 256), (256, 256), (512, 128), (384, 128)
PLANES = ("yz", "zy")
RING = ((0, 640), (640, 640))
UP = ((0, 256), (640, 384))
DOWN = ((256, 384), (1024, 256))
N_SEM = 116
N_MLP = 82
PIECES = (0, -1, 1, 2)
FORWARD = {1: (0, -1), -1: (1, 2)}
FORWARD_TWO = {1: (0,), -1: (1,)}


def place():
    dp, mp = lax.axis_index("dp"), lax.axis_index("mp")
    return {
        "x": lax.rem(dp // 2, 2) * 2 + mp // 4,
        "y": lax.rem(mp, 4),
        "z": dp // 4,
        "c": lax.rem(dp, 2),
    }


def device(p):
    return (p["z"] * 4 + (p["x"] // 2) * 2 + p["c"], lax.rem(p["x"], 2) * 4 + p["y"])


def shifted(p, dim, by):
    return {**p, dim: lax.rem(p[dim] + by + 4, 4)}


def other_core(p):
    return {**p, "c": 1 - p["c"]}


def slab(colour, phase, p, half=None):
    free = ORDERS[colour][: phase - 1]
    at = {"xl": lax.rem(p["x"], 2), "xh": p["x"] // 2, "y": p["y"], "z": p["z"], "r": ALL}
    for dim in free:
        for part in ("xl", "xh") if dim == "x" else (dim,):
            at[part] = ALL
    if half is not None:
        at["r"] = pl.ds(0, 48) if half == 0 else pl.ds(48, 32)
    return (at["xl"], at["y"], at["z"], at["xh"], p["c"], at["r"])


class Transfer:
    def __init__(self, owner, sent, received, lanes, target):
        number = owner.count
        owner.count += 1
        self.owner = owner

        def copy(where):
            ref = owner.ref.at[where + (pl.ds(*lanes),)]
            return pltpu.make_async_remote_copy(
                src_ref=ref,
                dst_ref=ref,
                send_sem=owner.send.at[number],
                recv_sem=owner.recv.at[number],
                device_id=device(target),
                device_id_type=MESH,
            )

        self.out, self.into = copy(sent), copy(received)

    def start(self):
        self.out.start()
        self.owner.started.append(self.out)

    def wait(self):
        self.into.wait_recv()


class Gather:
    def __init__(self, p, ref, send, recv):
        self.p, self.ref, self.send, self.recv = p, ref, send, recv
        self.count, self.started = 0, []

    def cross(self, piece, whole, dim, lanes, pieces, forward):
        p, mate = self.p, other_core(self.p)
        out = {"forward": forward}
        for way in (1, -1):
            target, source, far = shifted(p, dim, way), shifted(p, dim, -way), shifted(p, dim, 2)
            for r in pieces:
                out["full", way, r] = Transfer(self, piece(p, r), piece(source, r), lanes, target)
            for r in forward[way]:
                out["half", way, r] = Transfer(self, piece(source, r), piece(far, r), lanes, target)
        for way in (1, -1, 2):
            q = shifted(p, dim, way)
            out["mate", way] = Transfer(self, whole(q), whole(other_core(q)), lanes, mate)
        return out

    def offer(self, group, pieces):
        for r in pieces:
            for f in group:
                for way in (1, -1):
                    f["full", way, r].start()

    def relay(self, group, pieces):
        for r in pieces:
            for f in group:
                for way in (1, -1):
                    f["full", way, r].wait()
                    if r in f["forward"][way]:
                        f["half", way, r].start()

    def to_mate(self, group):
        for f in group:
            for way in (1, -1):
                f["mate", way].start()

    def last(self, group):
        for f in group:
            for way in (1, -1):
                for r in f["forward"][way]:
                    f["half", way, r].wait()

    def last_to_mate(self, group):
        for f in group:
            f["mate", 2].start()

    def all_from_mate(self, group):
        for f in group:
            for way in (1, -1, 2):
                f["mate", way].wait()

    def fulls(self, group):
        for f in group:
            f["full_up"].start()
            f["full_down"].start()

    def halves(self, group):
        for f in group:
            f["full_up"].wait()
            f["half_up"].start()
            f["full_down"].wait()
            f["half_down"].start()
        for f in group:
            f["mate_down"].start()
            f["mate_up"].start()

    def far(self, group):
        for f in group:
            f["half_up"].wait()
            f["half_down"].wait()

    def far_to_mate(self, group):
        for f in group:
            f["mate_far0"].start()
            f["mate_far1"].start()

    def from_mate(self, group):
        for f in group:
            for name in ("mate_down", "mate_up", "mate_far0", "mate_far1"):
                f[name].wait()


class Attention(Gather):
    def __init__(self, p, ref, send, recv):
        super().__init__(p, ref, send, recv)
        mate = other_core(p)
        self.own = Transfer(self, slab(0, 1, p), slab(0, 1, mate), (0, 640), mate)
        self.first = [self.ring(k, COLOURS[k]) for k in range(3)]
        self.second = [self.span(k, 2, COLOURS[k]) for k in range(3)]
        self.third = [self.span(k, 3, COLOURS[k]) for k in range(3)]

    def span(self, k, number, lanes):
        inner, dim = ORDERS[k][number - 2], ORDERS[k][number - 1]
        return self.cross(
            lambda q, r: slab(k, number - 1, shifted(q, inner, r)),
            lambda q: slab(k, number, q),
            dim,
            lanes,
            PIECES,
            FORWARD,
        )

    def ring(self, k, lanes):
        p = self.p
        dim = ORDERS[k][0]
        up, down, far = shifted(p, dim, 1), shifted(p, dim, -1), shifted(p, dim, 2)
        mate = other_core(p)

        def at(q, half=None):
            return slab(k, 1, q, half)

        def copy(sent, received, target):
            return Transfer(self, sent, received, lanes, target)

        return {
            "full_up": copy(at(p), at(down), up),
            "full_down": copy(at(p), at(up), down),
            "half_up": copy(at(down, 0), at(far, 0), up),
            "half_down": copy(at(up, 1), at(far, 1), down),
            "mate_down": copy(at(down), at(other_core(down)), mate),
            "mate_up": copy(at(up), at(other_core(up)), mate),
            "mate_far0": copy(at(far, 0), at(other_core(far), 0), mate),
            "mate_far1": copy(at(far, 1), at(other_core(far), 1), mate),
        }


class Mlp(Gather):
    def __init__(self, p, ref, send, recv):
        super().__init__(p, ref, send, recv)
        mate, over = other_core(p), shifted(p, "x", 2)
        whole = (0, 1280)
        self.own = Transfer(self, self.at(p), self.at(mate), whole, mate)
        self.over = Transfer(self, self.at(p), self.at(over), whole, over)
        self.over_mate = Transfer(self, self.at(over), self.at(other_core(over)), whole, mate)
        self.ring = [
            self.cross(
                lambda q, r: self.at(shifted(q, "x", 2 * r)),
                lambda q: self.at(q, "x"),
                PLANES[k][0],
                RING[k],
                (0, 1),
                FORWARD_TWO,
            )
            for k in range(2)
        ]
        self.up = [self.span(k, UP[k]) for k in range(2)]
        self.down = [self.span(k, DOWN[k]) for k in range(2)]

    def at(self, q, free=""):
        return (
            ALL if "y" in free else q["y"],
            ALL if "z" in free else q["z"],
            ALL if "x" in free else q["x"] // 2,
            q["c"],
            ALL,
        )

    def span(self, k, lanes):
        inner, dim = PLANES[k]
        return self.cross(
            lambda q, r: self.at(shifted(q, inner, r), "x"),
            lambda q: self.at(q, "x" + inner),
            dim,
            lanes,
            PIECES,
            FORWARD,
        )


def norm(values, gain, shift):
    mean = jnp.mean(values, axis=-1, keepdims=True)
    centred = values - mean
    spread = jnp.mean(centred * centred, axis=-1, keepdims=True)
    return (centred * lax.rsqrt(spread + 1e-06) * gain + shift).astype(BF)


def dot(a, b, contract=((1,), (0,))):
    return lax.dot_general(a, b, (contract, ((), ())), preferred_element_type=F32)


NT = ((1,), (1,))
TN = ((0,), (0,))


def kernel(
    patches,
    position,
    keep,
    counts,
    offsets,
    ln_gain,
    ln_bias,
    w_qkv,
    b_qkv,
    w_o,
    b_o,
    w_up,
    b_up,
    w_down,
    b_down,
    out,
    w,
    w_mlp,
    pictures,
    places,
    tokens,
    arrived,
    chosen,
    spread,
    slots,
    stream,
    normed,
    pair_rows,
    residual,
    hidden,
    partial,
    returned,
    biases,
    send,
    recv,
    send_mlp,
    recv_mlp,
    send_pair,
    recv_pair,
    load,
    send1,
    recv1,
    send1e,
    recv1e,
    sendb,
    recvb,
    send2,
    recv2,
    send2e,
    recv2e,
    send3,
    recv3,
    send3e,
    recv3e,
):
    dp, mp = lax.axis_index("dp"), lax.axis_index("mp")
    p = place()
    mate = other_core(p)
    tail_owner = (lax.rem(dp, 8), lax.rem(dp + 4, 8))
    has_tail = (mp == tail_owner[0]) | (mp == tail_owner[1])

    arrived[:, :, 128:256] = jnp.zeros((8, 256, 128), BF)

    barrier = pltpu.get_barrier_semaphore()

    def greet(target):
        pl.semaphore_signal(barrier, inc=1, device_id=target, device_id_type=MESH)

    for q in [shifted(p, d, s) for d in "xyz" for s in (1, -1)] + [mate]:
        greet(device(q))
    for k in range(1, 8):
        greet((dp, lax.rem(mp + k, 8)))
    for k in range(1, 16):
        greet((lax.rem(dp + k, 16), mp))

    load_pictures = pltpu.make_async_copy(patches, pictures, load.at[0])
    load_places = pltpu.make_async_copy(position, places, load.at[1])
    load_pictures.start()
    load_places.start()

    xl, xh = lax.rem(p["x"], 2), p["x"] // 2
    mine = (xl, p["y"], p["z"], xh, p["c"], ALL)

    def put(lane, value):
        w[mine + (pl.ds(lane, value.shape[1]),)] = value.astype(BF)

    def put_mlp(lane, value):
        w_mlp[mine[1:] + (pl.ds(lane, value.shape[1]),)] = value

    eye = (
        lax.broadcasted_iota(jnp.int32, (SLOT, SLOT), 0)
        == lax.broadcasted_iota(jnp.int32, (SLOT, SLOT), 1)
    ).astype(F32).astype(BF)
    out_t = dot(eye, w_o[0], NT)
    qkv = [w_qkv[0, t].astype(F32) for t in range(3)]
    put(0, qkv[0][:, :128])
    put(128, qkv[1][:, :128])
    put(256, qkv[2][:, :128])
    put(384, jnp.concatenate([v[:, 128:160] for v in qkv] + [out_t[:, 128:160]], axis=1))
    put(512, out_t[:, :128])
    put_mlp(0, w_up[0, :, 0:256])
    put_mlp(640, w_up[0, :, 256:640])
    put_mlp(256, w_down[0, :, 0:384])
    put_mlp(1024, w_down[0, :, 384:640])

    for t in range(3):
        biases[mp, t : t + 1, :] = b_qkv[t, 0:1, 0:128]
    biases[mp, 3:4, :] = jnp.concatenate(
        [b_qkv[t, 0:1, 128:160] for t in range(3)] + [jnp.zeros((1, 32), F32)], axis=1
    )
    for t in range(5):
        biases[mp, 4 + t : 5 + t, :] = b_up[0:1, t * 128 : (t + 1) * 128]

    pl.semaphore_wait(barrier, 29)

    g = Attention(p, w, send, recv)
    mlp = Mlp(p, w_mlp, send_mlp, recv_mlp)
    g.fulls(g.first)
    mlp.over.start()
    g.offer(g.second, (0,))
    mlp.offer(mlp.ring, (0,))
    g.own.start()
    mlp.own.start()

    load_pictures.wait()
    load_places.wait()
    for i in range(4):
        hit = lax.broadcasted_iota(jnp.int32, (256, KEEP), 0) == keep[i : i + 1, :]
        hit = hit.astype(F32).astype(BF)
        picked = dot(hit, pictures[i], TN) + dot(hit, places[...], TN)
        tokens[i * KEEP : (i + 1) * KEEP, :] = picked.astype(BF)

    def tile(k):
        return pl.ds(pl.multiple_of(k * 128, 128), 128)

    first_sends = []
    for k in range(1, 8):
        peer = lax.rem(mp + k, 8)
        for src, dst, s, r in (
            (tokens.at[:, tile(peer)], arrived.at[mp, :, pl.ds(0, 128)], send1, recv1),
            (biases.at[mp], biases.at[mp], sendb, recvb),
        ):
            copy = pltpu.make_async_remote_copy(
                src_ref=src,
                dst_ref=dst,
                send_sem=s.at[k],
                recv_sem=r.at[mp],
                device_id=(dp, peer),
                device_id_type=MESH,
            )
            copy.start()
            first_sends.append(copy)
    tail_sends = []
    for k in range(2):
        copy = pltpu.make_async_remote_copy(
            src_ref=tokens.at[:, pl.ds(1024 + 128 * k, 128)],
            dst_ref=arrived.at[mp, :, pl.ds(128, 128)],
            send_sem=send1e.at[k],
            recv_sem=recv1e.at[mp],
            device_id=(dp, tail_owner[k]),
            device_id_type=MESH,
        )
        tail_sends.append(copy)

        @pl.when(mp != tail_owner[k])
        def _():
            copy.start()

        @pl.when(mp == tail_owner[k])
        def _():
            arrived[mp, :, 128:256] = tokens[:, 1024 + 128 * k : 1152 + 128 * k]

    arrived[mp, :, 0:128] = tokens[:, tile(mp)]

    lane = lax.broadcasted_iota(jnp.int32, (16, 128), 1)
    inner = jnp.where(lane < KEEP, lane, lane - KEEP)
    pieces = []
    for k in range(16):
        a, b = dp * 32 + 2 * k, dp * 32 + 2 * k + 1
        count = jnp.where(lane < KEEP, counts[a], counts[b])
        start = jnp.where(lane < KEEP, offsets[a], offsets[b])
        pieces.append(jnp.where(inner < count, start + inner, -1))
    goal = jnp.concatenate(pieces, axis=1)
    sub = lax.broadcasted_iota(jnp.int32, (16, 2048), 0)

    def choose(i, carry):
        shard = i // 5
        row = shard * 1280 + dp * SLOT + (i - shard * 5) * 16
        hit = (goal - row) == sub
        chosen[pl.ds(pl.multiple_of(i * 16, 16), 16), :] = hit.astype(F32).astype(BF)
        return carry

    g.halves(g.first)
    g.offer(g.second, (-1, 1))
    lax.fori_loop(0, 40, choose, 0)

    g.far(g.first)
    g.offer(g.second, (2,))
    g.offer(g.third, (0,))
    g.far_to_mate(g.first)
    lax.fori_loop(40, 80, choose, 0)

    g.relay(g.second, (0, -1, 1))
    mlp.over.wait()
    mlp.offer(mlp.ring, (1,))
    mlp.over_mate.start()

    def wait_first(ref, sem, source):
        pltpu.make_async_remote_copy(
            src_ref=ref,
            dst_ref=ref,
            send_sem=send1.at[0],
            recv_sem=sem.at[source],
            device_id=(dp, source),
            device_id_type=MESH,
        ).wait_recv()

    for k in range(1, 8):
        source = lax.rem(mp + k, 8)
        wait_first(arrived.at[source, :, pl.ds(0, 128)], recv1, source)

    @pl.when(has_tail)
    def _():
        for k in range(1, 8):
            source = lax.rem(mp + k, 8)
            wait_first(arrived.at[source, :, pl.ds(128, 128)], recv1e, source)

    group = arrived[...].reshape(2048, 256)
    for k in range(4):
        rows = pl.ds(k * 320, 320)
        spread[rows, :] = dot(chosen[rows, :], group).astype(BF)

    def slot_rows(k):
        return pl.ds(pl.multiple_of(k * SLOT, 16), SLOT)

    second_sends = []
    for k in range(1, 16):
        shard = lax.rem(dp + k, 16)
        for extra in range(2):
            copy = pltpu.make_async_remote_copy(
                src_ref=spread.at[slot_rows(shard), pl.ds(128 * extra, 128)],
                dst_ref=slots.at[dp, :, pl.ds(128 * extra, 128)],
                send_sem=(send2e if extra else send2).at[k],
                recv_sem=(recv2e if extra else recv2).at[dp],
                device_id=(shard, mp),
                device_id_type=MESH,
            )
            if extra:
                pl.when(has_tail)(copy.start)
            else:
                copy.start()
            second_sends.append((copy, has_tail if extra else None))
    slots[dp] = spread[slot_rows(dp), :]

    g.relay(g.second, (2,))
    g.offer(g.third, (-1, 1))
    g.to_mate(g.second)
    mlp.relay(mlp.ring, (0, 1))
    mlp.to_mate(mlp.ring)
    mlp.offer(mlp.up, (0,))
    g.last(g.second)
    g.offer(g.third, (2,))
    g.last_to_mate(g.second)
    mlp.last(mlp.ring)
    mlp.last_to_mate(mlp.ring)

    def wait_copy(ref, sem):
        pltpu.make_async_remote_copy(
            src_ref=ref,
            dst_ref=ref,
            send_sem=send1.at[0],
            recv_sem=sem,
            device_id=device(mate),
            device_id_type=MESH,
        ).wait_recv()

    for k in range(1, 16):
        source = lax.rem(dp + k, 16)
        wait_copy(slots.at[source, :, pl.ds(0, 128)], recv2.at[source])
    third_sends = []
    for k in range(1, 8):
        peer = lax.rem(mp + k, 8)
        copy = pltpu.make_async_remote_copy(
            src_ref=slots.at[pl.ds(peer * 2, 2), :, pl.ds(0, 128)],
            dst_ref=stream.at[:, :, tile(mp)],
            send_sem=send3.at[k],
            recv_sem=recv3.at[mp],
            device_id=(dp, peer),
            device_id_type=MESH,
        )
        copy.start()
        third_sends.append((copy, None))
    stream[:, :, tile(mp)] = slots[pl.ds(mp * 2, 2), :, 0:128]
    for k in range(4):
        source = lax.rem(mp + 4 * k, 16)
        place_tail = pl.ds(1024 + 128 * (k % 2), 128)

        @pl.when(source != dp)
        def _():
            wait_copy(slots.at[source, :, pl.ds(128, 128)], recv2e.at[source])

        copy = pltpu.make_async_remote_copy(
            src_ref=slots.at[source, :, pl.ds(128, 128)],
            dst_ref=stream.at[lax.rem(source, 2), :, place_tail],
            send_sem=send3e.at[k],
            recv_sem=recv3e.at[lax.rem(source, 2), k % 2],
            device_id=(dp, source // 2),
            device_id_type=MESH,
        )
        away = source // 2 != mp
        pl.when(away)(copy.start)
        third_sends.append((copy, away))

        @pl.when(jnp.logical_not(away))
        def _():
            stream[lax.rem(source, 2), :, place_tail] = slots[source, :, 128:256]

    g.relay(g.third, PIECES)
    g.to_mate(g.third)
    mlp.offer(mlp.up, (-1, 1, 2))

    mlp.offer(mlp.down, PIECES)

    labels_row, labels_col = [], []
    for h in range(2):
        first = dp * 1280 + (mp * 2 + h) * SLOT
        down = first + lax.broadcasted_iota(jnp.int32, (SLOT, 128), 0)
        across = first + lax.broadcasted_iota(jnp.int32, (SLOT, 128), 1)

        def mark(i, carry):
            image = (mp * 2 + h) * 32 + i
            low = offsets[image]
            high = low + counts[image]
            return tuple(
                jnp.where((rows >= low) & (rows < high), i + 1, old)
                for rows, old in zip((down, across), carry)
            )

        zero = jnp.zeros((SLOT, 128), jnp.int32)
        col, row = lax.fori_loop(0, 32, mark, (zero, zero))
        labels_col.append(col)
        labels_row.append(row)
    same = [(labels_col[h] == labels_row[h])[:, :SLOT] for h in range(2)]
    used = jnp.concatenate([labels_col[h][:, 0:1] for h in range(2)], axis=0) > 0


    for k in range(1, 8):
        source = lax.rem(mp + k, 8)
        wait_copy(stream.at[:, :, tile(source)], recv3.at[source])
        wait_copy(biases.at[source], recvb.at[source])
    for h in range(2):
        for t in range(2):

            @pl.when(lax.rem(mp * 2 + h + 4 * t, 8) != mp)
            def _():
                wait_copy(stream.at[h, :, pl.ds(1024 + 128 * t, 128)], recv3e.at[h, t])

    rows_in = stream[...].reshape(ROWS, D).astype(F32)
    normed[...] = norm(rows_in, ln_gain[0, 0:1, :], ln_bias[0, 0:1, :])
    residual[...] = rows_in + b_o[...]

    g.last(g.third)
    g.last_to_mate(g.third)
    g.own.wait()
    g.from_mate(g.first)
    g.all_from_mate(g.second)
    g.all_from_mate(g.third)

    def weights(m, *lanes):
        parts = [w[m // 4, lax.rem(m, 4), :, :, :, :, pl.ds(*v)].reshape(D, v[1]) for v in lanes]
        return parts[0] if len(parts) == 1 else jnp.concatenate(parts, axis=1)

    def attention(m, carry):
        rows = normed[...]
        bias = biases[m]

        def projected(lanes, t):
            both = dot(rows, weights(m, lanes))
            return [both[:, 128 * i : 128 * (i + 1)] + bias[t + i : t + i + 1, :] for i in range(2)]

        q, k = projected(Q_K, 0)
        v, tail = projected(V_TAIL, 2)
        heads = []
        for i, value in enumerate((q, k, v)):
            second = jnp.concatenate([value[:, 80:128], tail[:, 32 * i : 32 * i + 32]], axis=1)
            heads.append((value[:, :80].astype(BF), second.astype(BF)))
        mixed = []
        for n in range(2):
            blocks = []
            for h in range(2):
                part = slice(h * SLOT, (h + 1) * SLOT)
                scores = dot(heads[0][n][part], heads[1][n][part], NT) * SCALE
                scores = jnp.where(same[h], scores, -jnp.inf)
                raised = jnp.exp(scores - jnp.max(scores, axis=-1, keepdims=True))
                share = (raised / jnp.sum(raised, axis=-1, keepdims=True)).astype(BF)
                blocks.append(dot(share, heads[2][n][part]))
            mixed.append(jnp.concatenate(blocks, axis=0))
        left = jnp.concatenate([mixed[0], mixed[1][:, :48]], axis=1).astype(BF)
        right = jnp.concatenate([jnp.zeros((ROWS, 96), F32), mixed[1][:, 48:]], axis=1).astype(BF)
        both = jnp.concatenate([left, right], axis=1)
        residual[...] += dot(both, weights(m, OUT, TAIL), NT)
        return carry

    lax.fori_loop(0, 4, attention, 0)
    mlp.relay(mlp.up, PIECES)
    mlp.to_mate(mlp.up)
    lax.fori_loop(4, 8, attention, 0)
    pair_rows[0:ROWS, :] = norm(residual[...], ln_gain[0, 1:2, :], ln_bias[0, 1:2, :])
    residual[...] += b_down[...]

    sides = (device(shifted(p, "x", 1)), device(shifted(p, "x", -1)))
    pair_sends = []

    def to_pair(src, dst, number, target):
        copy = pltpu.make_async_remote_copy(
            src_ref=src,
            dst_ref=dst,
            send_sem=send_pair.at[number],
            recv_sem=recv_pair.at[number],
            device_id=target,
            device_id_type=MESH,
        )
        copy.start()
        pair_sends.append(copy)

    for k in range(2):
        to_pair(
            pair_rows.at[pl.ds(SLOT * k, SLOT)],
            pair_rows.at[pl.ds(ROWS + SLOT * k, SLOT)],
            k,
            sides[k],
        )

    mlp.relay(mlp.down, PIECES)
    mlp.to_mate(mlp.down)
    mlp.last(mlp.up)
    mlp.last_to_mate(mlp.up)
    mlp.own.wait()
    mlp.over_mate.wait()
    mlp.all_from_mate(mlp.ring)
    mlp.all_from_mate(mlp.up)
    pair_sends[0].wait_recv()
    pair_sends[1].wait_recv()

    def up(y, carry):
        rows = pair_rows[...]
        bias = biases[xl * 4 + y]
        first = 0
        for lanes in UP:
            value = dot(rows, w_mlp[y, :, :, :, :, pl.ds(*lanes)].reshape(D, lanes[1]))
            tiles = lanes[1] // 128
            row = [bias[4 + first + i : 5 + first + i, :] for i in range(tiles)]
            value = value + jnp.concatenate(row, axis=1)
            value = 0.5 * value * (1.0 + lax.erf(value * (0.5**0.5)))
            hidden[y, :, first * 128 : (first + tiles) * 128] = value.astype(BF)
            first += tiles
        return carry

    lax.fori_loop(0, 4, up, 0)

    mlp.last(mlp.down)
    mlp.last_to_mate(mlp.down)
    mlp.all_from_mate(mlp.down)

    def down_weights(y, z, count):
        parts = [
            w_mlp[y, pl.ds(z, count), :, :, :, pl.ds(*v)].reshape(count * 320, v[1]) for v in DOWN
        ]
        return jnp.concatenate(parts, axis=1)

    for n in range(2):
        total = 0.0
        for y in range(4):
            total = total + dot(hidden[y, ROWS:, :], down_weights(y, 2 * n, 2), NT)
        columns = pl.ds(640 * n, 640)
        partial[:, columns] = total.astype(BF)
        for k in range(2):
            block = (pl.ds(SLOT * k, SLOT), columns)
            to_pair(partial.at[block], returned.at[block], 2 + 2 * n + k, sides[1 - k])

    def down(y, carry):
        residual[...] += dot(hidden[y, :ROWS, :], down_weights(y, 0, 4), NT)
        return carry

    lax.fori_loop(0, 4, down, 0)
    for n in range(4):
        pair_sends[2 + n].wait_recv()
    total = residual[...] + returned[...].astype(F32)
    out[...] = jnp.where(used, total, 0.0).astype(BF)

    for copy in g.started + mlp.started + first_sends + pair_sends:
        copy.wait_send()
    for k in range(2):
        pl.when(mp != tail_owner[k])(tail_sends[k].wait_send)
    for copy, away in second_sends + third_sends:
        if away is None:
            copy.wait_send()
        else:
            pl.when(away)(copy.wait_send)


def per_device(*args):
    args = list(args)
    args[8] = jnp.transpose(args[8], (1, 0, 2))
    args[13] = jnp.transpose(args[13], (0, 2, 1))
    vmem = pl.BlockSpec(memory_space=pltpu.VMEM)
    smem = pl.BlockSpec(memory_space=pltpu.SMEM)
    anywhere = pl.BlockSpec(memory_space=pl.ANY)
    specs = [anywhere, anywhere, vmem, smem, smem] + [vmem] * 10
    dma = pltpu.SemaphoreType.DMA
    return pl.pallas_call(
        kernel,
        out_shape=jax.ShapeDtypeStruct((ROWS, D), BF),
        in_specs=specs,
        out_specs=vmem,
        scratch_shapes=[
            pltpu.VMEM((2, 4, 4, 2, 2, SLOT, 640), BF),
            pltpu.VMEM((4, 4, 2, 2, SLOT, 1280), BF),
            pltpu.VMEM((4, 256, D), BF),
            pltpu.VMEM((256, D), BF),
            pltpu.VMEM((256, D), BF),
            pltpu.VMEM((8, 256, 256), BF),
            pltpu.VMEM((1280, 2048), BF),
            pltpu.VMEM((1280, 256), BF),
            pltpu.VMEM((16, SLOT, 256), BF),
            pltpu.VMEM((2, SLOT, D), BF),
            pltpu.VMEM((ROWS, D), BF),
            pltpu.VMEM((2 * ROWS, D), BF),
            pltpu.VMEM((ROWS, D), F32),
            pltpu.VMEM((4, 2 * ROWS, 640), BF),
            pltpu.VMEM((ROWS, D), BF),
            pltpu.VMEM((ROWS, D), BF),
            pltpu.VMEM((8, 16, 128), F32),
            dma((N_SEM,)),
            dma((N_SEM,)),
            dma((N_MLP,)),
            dma((N_MLP,)),
            dma((6,)),
            dma((6,)),
            dma((2,)),
            dma((8,)),
            dma((8,)),
            dma((2,)),
            dma((8,)),
            dma((8,)),
            dma((8,)),
            dma((16,)),
            dma((16,)),
            dma((16,)),
            dma((16,)),
            dma((8,)),
            dma((8,)),
            dma((4,)),
            dma((2, 2)),
        ],
        compiler_params=pltpu.CompilerParams(
            collective_id=0, has_side_effects=True, vmem_limit_bytes=62 * 1024 * 1024
        ),
        name="layer",
    )(*args)


def solution(mesh):
    in_specs = (
        P(("dp", "mp"), None, None),
        P(),
        P(("dp", "mp"), None),
        P(),
        P(),
        P(),
        P(),
        P(None, None, "dp", "mp"),
        P(None, None, "mp"),
        P(None, "mp", "dp"),
        P(),
        P(None, "dp", "mp"),
        P(None, "mp"),
        P(None, "mp", "dp"),
        P(),
    )
    return jax.shard_map(
        per_device,
        mesh=mesh,
        in_specs=in_specs,
        out_specs=P(("dp", "mp"), None),
        check_vma=False,
    )
```

```python
import jax
import jax.numpy as jnp
from jax import lax
from jax.experimental import pallas as pl
from jax.experimental.pallas import tpu as pltpu
from jax.sharding import PartitionSpec as P

BF = jnp.bfloat16
F32 = jnp.float32
MESH = pl.DeviceIdType.MESH
ALL = slice(None)
D = 1280
HEAD = 80
SLOT = 80
ROWS = 160
KEEP = 64
SCALE = 1.0 / HEAD**0.5

ORDERS = ("yxz", "zyx", "xzy")
COLOURS = ((0, 256), (256, 256), (512, 128))
Q_K, V_TAIL, OUT, TAIL = (0, 256), (256, 256), (512, 128), (384, 128)
PLANES = ("yz", "zy")
RING = ((0, 640), (640, 640))
UP = ((0, 256), (640, 384))
DOWN = ((256, 384), (1024, 256))
N_SEM = 116
N_MLP = 82
PIECES = (0, -1, 1, 2)
FORWARD = {1: (0, -1), -1: (1, 2)}
FORWARD_TWO = {1: (0,), -1: (1,)}


def place():
    dp, mp = lax.axis_index("dp"), lax.axis_index("mp")
    return {
        "x": lax.rem(dp // 2, 2) * 2 + mp // 4,
        "y": lax.rem(mp, 4),
        "z": dp // 4,
        "c": lax.rem(dp, 2),
    }


def device(p):
    return (p["z"] * 4 + (p["x"] // 2) * 2 + p["c"], lax.rem(p["x"], 2) * 4 + p["y"])


def shifted(p, dim, by):
    return {**p, dim: lax.rem(p[dim] + by + 4, 4)}


def other_core(p):
    return {**p, "c": 1 - p["c"]}


def slab(colour, phase, p, half=None):
    free = ORDERS[colour][: phase - 1]
    at = {"xl": lax.rem(p["x"], 2), "xh": p["x"] // 2, "y": p["y"], "z": p["z"], "r": ALL}
    for dim in free:
        for part in ("xl", "xh") if dim == "x" else (dim,):
            at[part] = ALL
    if half is not None:
        at["r"] = pl.ds(0, 48) if half == 0 else pl.ds(48, 32)
    return (at["xl"], at["y"], at["z"], at["xh"], p["c"], at["r"])


class Transfer:
    def __init__(self, owner, sent, received, lanes, target):
        number = owner.count
        owner.count += 1
        self.owner = owner

        def copy(where):
            ref = owner.ref.at[where + (pl.ds(*lanes),)]
            return pltpu.make_async_remote_copy(
                src_ref=ref,
                dst_ref=ref,
                send_sem=owner.send.at[number],
                recv_sem=owner.recv.at[number],
                device_id=device(target),
                device_id_type=MESH,
            )

        self.out, self.into = copy(sent), copy(received)

    def start(self):
        self.out.start()
        self.owner.started.append(self.out)

    def wait(self):
        self.into.wait_recv()


class Gather:
    def __init__(self, p, ref, send, recv):
        self.p, self.ref, self.send, self.recv = p, ref, send, recv
        self.count, self.started = 0, []

    def cross(self, piece, whole, dim, lanes, pieces, forward):
        p, mate = self.p, other_core(self.p)
        out = {"forward": forward}
        for way in (1, -1):
            target, source, far = shifted(p, dim, way), shifted(p, dim, -way), shifted(p, dim, 2)
            for r in pieces:
                out["full", way, r] = Transfer(self, piece(p, r), piece(source, r), lanes, target)
            for r in forward[way]:
                out["half", way, r] = Transfer(self, piece(source, r), piece(far, r), lanes, target)
        for way in (1, -1, 2):
            q = shifted(p, dim, way)
            out["mate", way] = Transfer(self, whole(q), whole(other_core(q)), lanes, mate)
        return out

    def offer(self, group, pieces):
        for r in pieces:
            for f in group:
                for way in (1, -1):
                    f["full", way, r].start()

    def relay(self, group, pieces):
        for r in pieces:
            for f in group:
                for way in (1, -1):
                    f["full", way, r].wait()
                    if r in f["forward"][way]:
                        f["half", way, r].start()

    def to_mate(self, group):
        for f in group:
            for way in (1, -1):
                f["mate", way].start()

    def last(self, group):
        for f in group:
            for way in (1, -1):
                for r in f["forward"][way]:
                    f["half", way, r].wait()

    def last_to_mate(self, group):
        for f in group:
            f["mate", 2].start()

    def all_from_mate(self, group):
        for f in group:
            for way in (1, -1, 2):
                f["mate", way].wait()

    def fulls(self, group):
        for f in group:
            f["full_up"].start()
            f["full_down"].start()

    def halves(self, group):
        for f in group:
            f["full_up"].wait()
            f["half_up"].start()
            f["full_down"].wait()
            f["half_down"].start()
        for f in group:
            f["mate_down"].start()
            f["mate_up"].start()

    def far(self, group):
        for f in group:
            f["half_up"].wait()
            f["half_down"].wait()

    def far_to_mate(self, group):
        for f in group:
            f["mate_far0"].start()
            f["mate_far1"].start()

    def from_mate(self, group):
        for f in group:
            for name in ("mate_down", "mate_up", "mate_far0", "mate_far1"):
                f[name].wait()


class Attention(Gather):
    def __init__(self, p, ref, send, recv):
        super().__init__(p, ref, send, recv)
        mate = other_core(p)
        self.own = Transfer(self, slab(0, 1, p), slab(0, 1, mate), (0, 640), mate)
        self.first = [self.ring(k, COLOURS[k]) for k in range(3)]
        self.second = [self.span(k, 2, COLOURS[k]) for k in range(3)]
        self.third = [self.span(k, 3, COLOURS[k]) for k in range(3)]

    def span(self, k, number, lanes):
        inner, dim = ORDERS[k][number - 2], ORDERS[k][number - 1]
        return self.cross(
            lambda q, r: slab(k, number - 1, shifted(q, inner, r)),
            lambda q: slab(k, number, q),
            dim,
            lanes,
            PIECES,
            FORWARD,
        )

    def ring(self, k, lanes):
        p = self.p
        dim = ORDERS[k][0]
        up, down, far = shifted(p, dim, 1), shifted(p, dim, -1), shifted(p, dim, 2)
        mate = other_core(p)

        def at(q, half=None):
            return slab(k, 1, q, half)

        def copy(sent, received, target):
            return Transfer(self, sent, received, lanes, target)

        return {
            "full_up": copy(at(p), at(down), up),
            "full_down": copy(at(p), at(up), down),
            "half_up": copy(at(down, 0), at(far, 0), up),
            "half_down": copy(at(up, 1), at(far, 1), down),
            "mate_down": copy(at(down), at(other_core(down)), mate),
            "mate_up": copy(at(up), at(other_core(up)), mate),
            "mate_far0": copy(at(far, 0), at(other_core(far), 0), mate),
            "mate_far1": copy(at(far, 1), at(other_core(far), 1), mate),
        }


class Mlp(Gather):
    def __init__(self, p, ref, send, recv):
        super().__init__(p, ref, send, recv)
        mate, over = other_core(p), shifted(p, "x", 2)
        whole = (0, 1280)
        self.own = Transfer(self, self.at(p), self.at(mate), whole, mate)
        self.over = Transfer(self, self.at(p), self.at(over), whole, over)
        self.over_mate = Transfer(self, self.at(over), self.at(other_core(over)), whole, mate)
        self.ring = [
            self.cross(
                lambda q, r: self.at(shifted(q, "x", 2 * r)),
                lambda q: self.at(q, "x"),
                PLANES[k][0],
                RING[k],
                (0, 1),
                FORWARD_TWO,
            )
            for k in range(2)
        ]
        self.up = [self.span(k, UP[k]) for k in range(2)]
        self.down = [self.span(k, DOWN[k]) for k in range(2)]

    def at(self, q, free=""):
        return (
            ALL if "y" in free else q["y"],
            ALL if "z" in free else q["z"],
            ALL if "x" in free else q["x"] // 2,
            q["c"],
            ALL,
        )

    def span(self, k, lanes):
        inner, dim = PLANES[k]
        return self.cross(
            lambda q, r: self.at(shifted(q, inner, r), "x"),
            lambda q: self.at(q, "x" + inner),
            dim,
            lanes,
            PIECES,
            FORWARD,
        )


def norm(values, gain, shift):
    mean = jnp.mean(values, axis=-1, keepdims=True)
    centred = values - mean
    spread = jnp.mean(centred * centred, axis=-1, keepdims=True)
    return (centred * lax.rsqrt(spread + 1e-06) * gain + shift).astype(BF)


def dot(a, b, contract=((1,), (0,))):
    return lax.dot_general(a, b, (contract, ((), ())), preferred_element_type=F32)


NT = ((1,), (1,))
TN = ((0,), (0,))


def kernel(
    patches,
    position,
    keep,
    counts,
    offsets,
    ln_gain,
    ln_bias,
    w_qkv,
    b_qkv,
    w_o,
    b_o,
    w_up,
    b_up,
    w_down,
    b_down,
    out,
    w,
    w_mlp,
    pictures,
    places,
    tokens,
    arrived,
    chosen,
    spread,
    slots,
    stream,
    normed,
    pair_rows,
    residual,
    hidden,
    partial,
    returned,
    biases,
    send,
    recv,
    send_mlp,
    recv_mlp,
    send_pair,
    recv_pair,
    load,
    send1,
    recv1,
    send1e,
    recv1e,
    sendb,
    recvb,
    send2,
    recv2,
    send2e,
    recv2e,
    send3,
    recv3,
    send3e,
    recv3e,
):
    dp, mp = lax.axis_index("dp"), lax.axis_index("mp")
    p = place()
    mate = other_core(p)
    tail_owner = (lax.rem(dp, 8), lax.rem(dp + 4, 8))
    has_tail = (mp == tail_owner[0]) | (mp == tail_owner[1])

    arrived[:, :, 128:256] = jnp.zeros((8, 256, 128), BF)

    barrier = pltpu.get_barrier_semaphore()

    def greet(target):
        pl.semaphore_signal(barrier, inc=1, device_id=target, device_id_type=MESH)

    for q in [shifted(p, d, s) for d in "xyz" for s in (1, -1)] + [mate]:
        greet(device(q))
    for k in range(1, 8):
        greet((dp, lax.rem(mp + k, 8)))
    for k in range(1, 16):
        greet((lax.rem(dp + k, 16), mp))

    load_pictures = pltpu.make_async_copy(patches, pictures, load.at[0])
    load_places = pltpu.make_async_copy(position, places, load.at[1])
    load_pictures.start()
    load_places.start()

    xl, xh = lax.rem(p["x"], 2), p["x"] // 2
    mine = (xl, p["y"], p["z"], xh, p["c"], ALL)

    def put(lane, value):
        w[mine + (pl.ds(lane, value.shape[1]),)] = value.astype(BF)

    def put_mlp(lane, value):
        w_mlp[mine[1:] + (pl.ds(lane, value.shape[1]),)] = value

    eye = (
        lax.broadcasted_iota(jnp.int32, (SLOT, SLOT), 0)
        == lax.broadcasted_iota(jnp.int32, (SLOT, SLOT), 1)
    ).astype(F32).astype(BF)
    out_t = dot(eye, w_o[0], NT)
    qkv = [w_qkv[0, t].astype(F32) for t in range(3)]
    put(0, qkv[0][:, :128])
    put(128, qkv[1][:, :128])
    put(256, qkv[2][:, :128])
    put(384, jnp.concatenate([v[:, 128:160] for v in qkv] + [out_t[:, 128:160]], axis=1))
    put(512, out_t[:, :128])
    put_mlp(0, w_up[0, :, 0:256])
    put_mlp(640, w_up[0, :, 256:640])
    put_mlp(256, w_down[0, :, 0:384])
    put_mlp(1024, w_down[0, :, 384:640])

    for t in range(3):
        biases[mp, t : t + 1, :] = b_qkv[t, 0:1, 0:128]
    biases[mp, 3:4, :] = jnp.concatenate(
        [b_qkv[t, 0:1, 128:160] for t in range(3)] + [jnp.zeros((1, 32), F32)], axis=1
    )
    for t in range(5):
        biases[mp, 4 + t : 5 + t, :] = b_up[0:1, t * 128 : (t + 1) * 128]

    pl.semaphore_wait(barrier, 29)

    g = Attention(p, w, send, recv)
    mlp = Mlp(p, w_mlp, send_mlp, recv_mlp)
    g.fulls(g.first)
    mlp.over.start()
    g.offer(g.second, (0,))
    mlp.offer(mlp.ring, (0,))
    g.own.start()
    mlp.own.start()

    load_pictures.wait()
    load_places.wait()
    for i in range(4):
        hit = lax.broadcasted_iota(jnp.int32, (256, KEEP), 0) == keep[i : i + 1, :]
        hit = hit.astype(F32).astype(BF)
        picked = dot(hit, pictures[i], TN) + dot(hit, places[...], TN)
        tokens[i * KEEP : (i + 1) * KEEP, :] = picked.astype(BF)

    def tile(k):
        return pl.ds(pl.multiple_of(k * 128, 128), 128)

    first_sends = []
    for k in range(1, 8):
        peer = lax.rem(mp + k, 8)
        for src, dst, s, r in (
            (tokens.at[:, tile(peer)], arrived.at[mp, :, pl.ds(0, 128)], send1, recv1),
            (biases.at[mp], biases.at[mp], sendb, recvb),
        ):
            copy = pltpu.make_async_remote_copy(
                src_ref=src,
                dst_ref=dst,
                send_sem=s.at[k],
                recv_sem=r.at[mp],
                device_id=(dp, peer),
                device_id_type=MESH,
            )
            copy.start()
            first_sends.append(copy)
    tail_sends = []
    for k in range(2):
        copy = pltpu.make_async_remote_copy(
            src_ref=tokens.at[:, pl.ds(1024 + 128 * k, 128)],
            dst_ref=arrived.at[mp, :, pl.ds(128, 128)],
            send_sem=send1e.at[k],
            recv_sem=recv1e.at[mp],
            device_id=(dp, tail_owner[k]),
            device_id_type=MESH,
        )
        tail_sends.append(copy)

        @pl.when(mp != tail_owner[k])
        def _():
            copy.start()

        @pl.when(mp == tail_owner[k])
        def _():
            arrived[mp, :, 128:256] = tokens[:, 1024 + 128 * k : 1152 + 128 * k]

    arrived[mp, :, 0:128] = tokens[:, tile(mp)]

    lane = lax.broadcasted_iota(jnp.int32, (16, 128), 1)
    inner = jnp.where(lane < KEEP, lane, lane - KEEP)
    pieces = []
    for k in range(16):
        a, b = dp * 32 + 2 * k, dp * 32 + 2 * k + 1
        count = jnp.where(lane < KEEP, counts[a], counts[b])
        start = jnp.where(lane < KEEP, offsets[a], offsets[b])
        pieces.append(jnp.where(inner < count, start + inner, -1))
    goal = jnp.concatenate(pieces, axis=1)
    sub = lax.broadcasted_iota(jnp.int32, (16, 2048), 0)

    def choose(i, carry):
        shard = i // 5
        row = shard * 1280 + dp * SLOT + (i - shard * 5) * 16
        hit = (goal - row) == sub
        chosen[pl.ds(pl.multiple_of(i * 16, 16), 16), :] = hit.astype(F32).astype(BF)
        return carry

    g.halves(g.first)
    g.offer(g.second, (-1, 1))
    lax.fori_loop(0, 40, choose, 0)

    g.far(g.first)
    g.offer(g.second, (2,))
    g.offer(g.third, (0,))
    g.far_to_mate(g.first)
    lax.fori_loop(40, 80, choose, 0)

    g.relay(g.second, (0, -1, 1))
    mlp.over.wait()
    mlp.offer(mlp.ring, (1,))
    mlp.over_mate.start()

    def wait_first(ref, sem, source):
        pltpu.make_async_remote_copy(
            src_ref=ref,
            dst_ref=ref,
            send_sem=send1.at[0],
            recv_sem=sem.at[source],
            device_id=(dp, source),
            device_id_type=MESH,
        ).wait_recv()

    for k in range(1, 8):
        source = lax.rem(mp + k, 8)
        wait_first(arrived.at[source, :, pl.ds(0, 128)], recv1, source)

    @pl.when(has_tail)
    def _():
        for k in range(1, 8):
            source = lax.rem(mp + k, 8)
            wait_first(arrived.at[source, :, pl.ds(128, 128)], recv1e, source)

    group = arrived[...].reshape(2048, 256)
    for k in range(4):
        rows = pl.ds(k * 320, 320)
        spread[rows, :] = dot(chosen[rows, :], group).astype(BF)

    def slot_rows(k):
        return pl.ds(pl.multiple_of(k * SLOT, 16), SLOT)

    second_sends = []
    for k in range(1, 16):
        shard = lax.rem(dp + k, 16)
        for extra in range(2):
            copy = pltpu.make_async_remote_copy(
                src_ref=spread.at[slot_rows(shard), pl.ds(128 * extra, 128)],
                dst_ref=slots.at[dp, :, pl.ds(128 * extra, 128)],
                send_sem=(send2e if extra else send2).at[k],
                recv_sem=(recv2e if extra else recv2).at[dp],
                device_id=(shard, mp),
                device_id_type=MESH,
            )
            if extra:
                pl.when(has_tail)(copy.start)
            else:
                copy.start()
            second_sends.append((copy, has_tail if extra else None))
    slots[dp] = spread[slot_rows(dp), :]

    g.relay(g.second, (2,))
    g.offer(g.third, (-1, 1))
    g.to_mate(g.second)
    mlp.relay(mlp.ring, (0, 1))
    mlp.to_mate(mlp.ring)
    mlp.offer(mlp.up, (0,))
    g.last(g.second)
    g.offer(g.third, (2,))
    g.last_to_mate(g.second)
    mlp.last(mlp.ring)
    mlp.last_to_mate(mlp.ring)

    def wait_copy(ref, sem):
        pltpu.make_async_remote_copy(
            src_ref=ref,
            dst_ref=ref,
            send_sem=send1.at[0],
            recv_sem=sem,
            device_id=device(mate),
            device_id_type=MESH,
        ).wait_recv()

    for k in range(1, 16):
        source = lax.rem(dp + k, 16)
        wait_copy(slots.at[source, :, pl.ds(0, 128)], recv2.at[source])
    third_sends = []
    for k in range(1, 8):
        peer = lax.rem(mp + k, 8)
        copy = pltpu.make_async_remote_copy(
            src_ref=slots.at[pl.ds(peer * 2, 2), :, pl.ds(0, 128)],
            dst_ref=stream.at[:, :, tile(mp)],
            send_sem=send3.at[k],
            recv_sem=recv3.at[mp],
            device_id=(dp, peer),
            device_id_type=MESH,
        )
        copy.start()
        third_sends.append((copy, None))
    stream[:, :, tile(mp)] = slots[pl.ds(mp * 2, 2), :, 0:128]
    for k in range(4):
        source = lax.rem(mp + 4 * k, 16)
        place_tail = pl.ds(1024 + 128 * (k % 2), 128)

        @pl.when(source != dp)
        def _():
            wait_copy(slots.at[source, :, pl.ds(128, 128)], recv2e.at[source])

        copy = pltpu.make_async_remote_copy(
            src_ref=slots.at[source, :, pl.ds(128, 128)],
            dst_ref=stream.at[lax.rem(source, 2), :, place_tail],
            send_sem=send3e.at[k],
            recv_sem=recv3e.at[lax.rem(source, 2), k % 2],
            device_id=(dp, source // 2),
            device_id_type=MESH,
        )
        away = source // 2 != mp
        pl.when(away)(copy.start)
        third_sends.append((copy, away))

        @pl.when(jnp.logical_not(away))
        def _():
            stream[lax.rem(source, 2), :, place_tail] = slots[source, :, 128:256]

    g.relay(g.third, PIECES)
    g.to_mate(g.third)
    mlp.offer(mlp.up, (-1, 1, 2))

    mlp.offer(mlp.down, PIECES)

    labels_row, labels_col = [], []
    for h in range(2):
        first = dp * 1280 + (mp * 2 + h) * SLOT
        down = first + lax.broadcasted_iota(jnp.int32, (SLOT, 128), 0)
        across = first + lax.broadcasted_iota(jnp.int32, (SLOT, 128), 1)

        def mark(i, carry):
            image = (mp * 2 + h) * 32 + i
            low = offsets[image]
            high = low + counts[image]
            return tuple(
                jnp.where((rows >= low) & (rows < high), i + 1, old)
                for rows, old in zip((down, across), carry)
            )

        zero = jnp.zeros((SLOT, 128), jnp.int32)
        col, row = lax.fori_loop(0, 32, mark, (zero, zero))
        labels_col.append(col)
        labels_row.append(row)
    same = [(labels_col[h] == labels_row[h])[:, :SLOT] for h in range(2)]
    used = jnp.concatenate([labels_col[h][:, 0:1] for h in range(2)], axis=0) > 0


    for k in range(1, 8):
        source = lax.rem(mp + k, 8)
        wait_copy(stream.at[:, :, tile(source)], recv3.at[source])
        wait_copy(biases.at[source], recvb.at[source])
    for h in range(2):
        for t in range(2):

            @pl.when(lax.rem(mp * 2 + h + 4 * t, 8) != mp)
            def _():
                wait_copy(stream.at[h, :, pl.ds(1024 + 128 * t, 128)], recv3e.at[h, t])

    rows_in = stream[...].reshape(ROWS, D).astype(F32)
    normed[...] = norm(rows_in, ln_gain[0, 0:1, :], ln_bias[0, 0:1, :])
    residual[...] = rows_in + b_o[...]

    g.last(g.third)
    g.last_to_mate(g.third)
    g.own.wait()
    g.from_mate(g.first)
    g.all_from_mate(g.second)
    g.all_from_mate(g.third)

    def weights(m, *lanes):
        parts = [w[m // 4, lax.rem(m, 4), :, :, :, :, pl.ds(*v)].reshape(D, v[1]) for v in lanes]
        return parts[0] if len(parts) == 1 else jnp.concatenate(parts, axis=1)

    def attention(m, carry):
        rows = normed[...]
        bias = biases[m]

        def projected(lanes, t):
            both = dot(rows, weights(m, lanes))
            return [both[:, 128 * i : 128 * (i + 1)] + bias[t + i : t + i + 1, :] for i in range(2)]

        q, k = projected(Q_K, 0)
        v, tail = projected(V_TAIL, 2)
        heads = []
        for i, value in enumerate((q, k, v)):
            second = jnp.concatenate([value[:, 80:128], tail[:, 32 * i : 32 * i + 32]], axis=1)
            heads.append((value[:, :80].astype(BF), second.astype(BF)))
        mixed = []
        for n in range(2):
            blocks = []
            for h in range(2):
                part = slice(h * SLOT, (h + 1) * SLOT)
                scores = dot(heads[0][n][part], heads[1][n][part], NT) * SCALE
                scores = jnp.where(same[h], scores, -jnp.inf)
                raised = jnp.exp(scores - jnp.max(scores, axis=-1, keepdims=True))
                share = (raised / jnp.sum(raised, axis=-1, keepdims=True)).astype(BF)
                blocks.append(dot(share, heads[2][n][part]))
            mixed.append(jnp.concatenate(blocks, axis=0))
        left = jnp.concatenate([mixed[0], mixed[1][:, :48]], axis=1).astype(BF)
        right = jnp.concatenate([jnp.zeros((ROWS, 96), F32), mixed[1][:, 48:]], axis=1).astype(BF)
        both = jnp.concatenate([left, right], axis=1)
        residual[...] += dot(both, weights(m, OUT, TAIL), NT)
        return carry

    lax.fori_loop(0, 4, attention, 0)
    mlp.relay(mlp.up, PIECES)
    mlp.to_mate(mlp.up)
    lax.fori_loop(4, 8, attention, 0)
    pair_rows[0:ROWS, :] = norm(residual[...], ln_gain[0, 1:2, :], ln_bias[0, 1:2, :])
    residual[...] += b_down[...]

    sides = (device(shifted(p, "x", 1)), device(shifted(p, "x", -1)))
    pair_sends = []

    def to_pair(src, dst, number, target):
        copy = pltpu.make_async_remote_copy(
            src_ref=src,
            dst_ref=dst,
            send_sem=send_pair.at[number],
            recv_sem=recv_pair.at[number],
            device_id=target,
            device_id_type=MESH,
        )
        copy.start()
        pair_sends.append(copy)

    for k in range(2):
        to_pair(
            pair_rows.at[pl.ds(SLOT * k, SLOT)],
            pair_rows.at[pl.ds(ROWS + SLOT * k, SLOT)],
            k,
            sides[k],
        )

    mlp.relay(mlp.down, PIECES)
    mlp.to_mate(mlp.down)
    mlp.last(mlp.up)
    mlp.last_to_mate(mlp.up)
    mlp.own.wait()
    mlp.over_mate.wait()
    mlp.all_from_mate(mlp.ring)
    mlp.all_from_mate(mlp.up)
    pair_sends[0].wait_recv()
    pair_sends[1].wait_recv()

    def up(y, carry):
        rows = pair_rows[...]
        bias = biases[xl * 4 + y]
        first = 0
        for lanes in UP:
            value = dot(rows, w_mlp[y, :, :, :, :, pl.ds(*lanes)].reshape(D, lanes[1]))
            tiles = lanes[1] // 128
            row = [bias[4 + first + i : 5 + first + i, :] for i in range(tiles)]
            value = value + jnp.concatenate(row, axis=1)
            value = 0.5 * value * (1.0 + lax.erf(value * (0.5**0.5)))
            hidden[y, :, first * 128 : (first + tiles) * 128] = value.astype(BF)
            first += tiles
        return carry

    lax.fori_loop(0, 4, up, 0, unroll=2)

    mlp.last(mlp.down)
    mlp.last_to_mate(mlp.down)
    mlp.all_from_mate(mlp.down)

    def down_weights(y, z, count):
        parts = [
            w_mlp[y, pl.ds(z, count), :, :, :, pl.ds(*v)].reshape(count * 320, v[1]) for v in DOWN
        ]
        return jnp.concatenate(parts, axis=1)

    for n in range(2):
        total = 0.0
        for y in range(4):
            total = total + dot(hidden[y, ROWS:, :], down_weights(y, 2 * n, 2), NT)
        columns = pl.ds(640 * n, 640)
        partial[:, columns] = total.astype(BF)
        for k in range(2):
            block = (pl.ds(SLOT * k, SLOT), columns)
            to_pair(partial.at[block], returned.at[block], 2 + 2 * n + k, sides[1 - k])

    def down(y, carry):
        residual[...] += dot(hidden[y, :ROWS, :], down_weights(y, 0, 4), NT)
        return carry

    lax.fori_loop(0, 4, down, 0, unroll=2)
    for n in range(4):
        pair_sends[2 + n].wait_recv()
    total = residual[...] + returned[...].astype(F32)
    out[...] = jnp.where(used, total, 0.0).astype(BF)

    for copy in g.started + mlp.started + first_sends + pair_sends:
        copy.wait_send()
    for k in range(2):
        pl.when(mp != tail_owner[k])(tail_sends[k].wait_send)
    for copy, away in second_sends + third_sends:
        if away is None:
            copy.wait_send()
        else:
            pl.when(away)(copy.wait_send)


def per_device(*args):
    args = list(args)
    args[8] = jnp.transpose(args[8], (1, 0, 2))
    args[13] = jnp.transpose(args[13], (0, 2, 1))
    vmem = pl.BlockSpec(memory_space=pltpu.VMEM)
    smem = pl.BlockSpec(memory_space=pltpu.SMEM)
    anywhere = pl.BlockSpec(memory_space=pl.ANY)
    specs = [anywhere, anywhere, vmem, smem, smem] + [vmem] * 10
    dma = pltpu.SemaphoreType.DMA
    return pl.pallas_call(
        kernel,
        out_shape=jax.ShapeDtypeStruct((ROWS, D), BF),
        in_specs=specs,
        out_specs=vmem,
        scratch_shapes=[
            pltpu.VMEM((2, 4, 4, 2, 2, SLOT, 640), BF),
            pltpu.VMEM((4, 4, 2, 2, SLOT, 1280), BF),
            pltpu.VMEM((4, 256, D), BF),
            pltpu.VMEM((256, D), BF),
            pltpu.VMEM((256, D), BF),
            pltpu.VMEM((8, 256, 256), BF),
            pltpu.VMEM((1280, 2048), BF),
            pltpu.VMEM((1280, 256), BF),
            pltpu.VMEM((16, SLOT, 256), BF),
            pltpu.VMEM((2, SLOT, D), BF),
            pltpu.VMEM((ROWS, D), BF),
            pltpu.VMEM((2 * ROWS, D), BF),
            pltpu.VMEM((ROWS, D), F32),
            pltpu.VMEM((4, 2 * ROWS, 640), BF),
            pltpu.VMEM((ROWS, D), BF),
            pltpu.VMEM((ROWS, D), BF),
            pltpu.VMEM((8, 16, 128), F32),
            dma((N_SEM,)),
            dma((N_SEM,)),
            dma((N_MLP,)),
            dma((N_MLP,)),
            dma((6,)),
            dma((6,)),
            dma((2,)),
            dma((8,)),
            dma((8,)),
            dma((2,)),
            dma((8,)),
            dma((8,)),
            dma((8,)),
            dma((16,)),
            dma((16,)),
            dma((16,)),
            dma((16,)),
            dma((8,)),
            dma((8,)),
            dma((4,)),
            dma((2, 2)),
        ],
        compiler_params=pltpu.CompilerParams(
            collective_id=0, has_side_effects=True, vmem_limit_bytes=62 * 1024 * 1024
        ),
        name="layer",
    )(*args)


def solution(mesh):
    in_specs = (
        P(("dp", "mp"), None, None),
        P(),
        P(("dp", "mp"), None),
        P(),
        P(),
        P(),
        P(),
        P(None, None, "dp", "mp"),
        P(None, None, "mp"),
        P(None, "mp", "dp"),
        P(),
        P(None, "dp", "mp"),
        P(None, "mp"),
        P(None, "mp", "dp"),
        P(),
    )
    return jax.shard_map(
        per_device,
        mesh=mesh,
        in_specs=in_specs,
        out_specs=P(("dp", "mp"), None),
        check_vma=False,
    )
```
